32 devices in a mesh: face: 4 (over z), tile: 4 (over y, core), lev: 2 (over x).
Axes of the slice: x: 2, y: 2, z: 4, core: 2. Of those that a mesh axis runs over, the one named last changes fastest.
Arguments:
- airflow_components: float32 [2, 36, 32, 512], P(None, 'lev', 'face', 'tile'), may hold values from -4.5 to 4.5, as said below
- heat_state: float32 [36, 32, 512], P('lev', 'face', 'tile'), may hold values from 0.5 to 2
- layer_pressure_depth: float32 [36, 32, 512], P('lev', 'face', 'tile'), may hold values from 0.5 to 2
- constituent_masses: float32 [18, 36, 32, 512], P(None, 'lev', 'face', 'tile'), may hold values from 0.1 to 1
- ground_gravity_potential: float32 [32, 512], P('face', 'tile'), may hold values from -8 to 8
- inverse_mapping_entries: float32 [4, 32, 512], P(None, 'face', 'tile'), may hold values from -4 to 4
- mapping_determinant: float32 [32, 512], P('face', 'tile'), may hold values from 0.5 to 2
- interface_rightangle_rotations: int32 [4, 4, 2], replicated, may hold values from 0 to 3
- interface_flipped_markers: int32 [4, 4, 2], replicated, may hold values from 0 to 1
- corner_block_tally: int32 [4, 4], replicated, may hold values from 3 to 4
Outputs:
- airflow_next: float32 [2, 36, 32, 512], P(None, 'lev', 'face', 'tile')
- heat_state_next: float32 [36, 32, 512], P('lev', 'face', 'tile')
- pressure_depth_next: float32 [36, 32, 512], P('lev', 'face', 'tile')
- constituent_masses_next: float32 [18, 36, 32, 512], P(None, 'lev', 'face', 'tile')
- stepping_bounds: float32 [2], replicated
The draws below stay inside these ranges and needn't reach their ends.
Inputs may be any that keep to these rules, and one draw needn't show every extreme that they name: `airflow_components`: component magnitudes grow across the grid by up to a factor of 9. `interface_rightangle_rotations`: entry [f, t, 0] concerns the boundary between blocks (f, t) and (f+1, t), entry [f, t, 1] the one between (f, t) and (f, t+1). `interface_flipped_markers`: indexed like interface_rightangle_rotations. `corner_block_tally`: entry [f, t] belongs to the corner shared by blocks (f, t), (f+1, t), (f, t+1), (f+1, t+1).
All inputs are finite; a program needn't handle non-finite values.
Results may differ from the reference program's by a relative error of at most 0.00012.
Values sent between devices are 32-bit elements; how exact they have to be, the bound alone decides.
A program may use at most 64 MiB of HBM per device.

```python
import math
import jax
import jax.numpy as jnp
import numpy as np
from jax import lax

QSIZE = 18
MESH_NODE_NORTHS = 32
MESH_NODE_EASTS = 512
LAYER_NUMBER = 36
N_FACE = 4
N_TILE = 4


def draw_airflow_components(key, part):
    row_position = jnp.arange(MESH_NODE_NORTHS, dtype=jnp.float32)[:, None] / MESH_NODE_NORTHS
    column_position = jnp.arange(MESH_NODE_EASTS, dtype=jnp.float32)[None, :] / MESH_NODE_EASTS
    spread_factor = 0.5 * jnp.exp(jnp.log(3.0) * (row_position + column_position))
    standard = jnp.clip(jax.random.normal(key, (2, LAYER_NUMBER, MESH_NODE_NORTHS, MESH_NODE_EASTS), jnp.float32), -3.0, 3.0)
    return (standard * spread_factor / 3.0).astype(jnp.float32)


def touch_ends(drawn, stream_key, smallest, largest):
    longest = drawn.shape.index(max(drawn.shape))
    spots = []
    for shift in (0, 1):
        where = [jax.random.randint(jax.random.fold_in(stream_key, axis), (), 0, length) for axis, length in enumerate(drawn.shape)]
        where[longest] = (where[longest] + shift) % drawn.shape[longest]
        spots.append(tuple(where))
    return drawn.at[spots[0]].set(smallest).at[spots[1]].set(largest)


def steps_of(rng, shape, cuts, low, largest):
    def one(position, blocks):
        heights = jax.random.uniform(jax.random.fold_in(jax.random.fold_in(rng, 6), position), (blocks,), jnp.float32, low / len(cuts), largest / len(cuts))
        return jnp.repeat(jnp.exp(heights), shape[position] // blocks).reshape((-1,) + (1,) * (len(shape) - position - 1))

    level = one(*cuts[0])
    for cut in cuts[1:]:
        level = level * one(*cut)
    return level


def noise(key, extent, spread, bound, split=(), kind=jnp.bfloat16):
    result = spread * jax.random.normal(key, extent, jnp.float32)
    if split:
        result = result * steps_of(key, extent, split, -0.22, 0.18)
    return jnp.clip(result, -bound, bound).astype(kind)


def setup_inputs(seed: int = 0) -> dict:
    splits = jax.random.split(jax.random.key(seed), 11)
    airflow_components = draw_airflow_components(jax.random.fold_in(splits[10], 71), 0)
    heat_state = jnp.clip(jnp.exp(math.log(2.0) - 1.3862944 * jax.random.uniform(splits[1], (LAYER_NUMBER, MESH_NODE_NORTHS, MESH_NODE_EASTS), jnp.float32) ** steps_of(splits[1], (LAYER_NUMBER, MESH_NODE_NORTHS, MESH_NODE_EASTS), ((0, 2), (1, 4), (2, 4)), -0.2, 0.2)), 0.5, 2.0)
    layer_pressure_depth = jnp.clip(jnp.exp(math.log(2.0) - 1.3862944 * jax.random.uniform(splits[2], (LAYER_NUMBER, MESH_NODE_NORTHS, MESH_NODE_EASTS), jnp.float32) ** steps_of(splits[2], (LAYER_NUMBER, MESH_NODE_NORTHS, MESH_NODE_EASTS), ((0, 2), (1, 4), (2, 4)), -0.2, 0.2)), 0.5, 2.0)
    constituent_masses = jnp.clip(jnp.exp(math.log(1.0) - 2.3025851 * jax.random.uniform(splits[3], (QSIZE, LAYER_NUMBER, MESH_NODE_NORTHS, MESH_NODE_EASTS), jnp.float32) ** steps_of(splits[3], (QSIZE, LAYER_NUMBER, MESH_NODE_NORTHS, MESH_NODE_EASTS), ((1, 2), (2, 4), (3, 4)), -0.2, 0.2)), 0.1, 1.0)
    ground_gravity_potential = noise(splits[4], (MESH_NODE_NORTHS, MESH_NODE_EASTS), 2.0, 8.0, ((0, 4), (1, 4)), jnp.float32)
    inverse_mapping_entries = noise(splits[5], (4, MESH_NODE_NORTHS, MESH_NODE_EASTS), 1.0, 4.0, ((1, 4), (2, 4)), jnp.float32)
    mapping_determinant = jnp.clip(jnp.exp(math.log(2.0) - 1.3862944 * jax.random.uniform(splits[6], (MESH_NODE_NORTHS, MESH_NODE_EASTS), jnp.float32) ** steps_of(splits[6], (MESH_NODE_NORTHS, MESH_NODE_EASTS), ((0, 4), (1, 4)), -0.2, 0.2)), 0.5, 2.0)
    interface_rightangle_rotations = touch_ends(jax.random.randint(splits[7], (N_FACE, N_TILE, 2), 0, 4), jax.random.fold_in(splits[7], 1), 0, 3).astype(jnp.int32)
    interface_flipped_markers = touch_ends(jax.random.randint(splits[8], (N_FACE, N_TILE, 2), 0, 2), jax.random.fold_in(splits[8], 1), 0, 1).astype(jnp.int32)
    corner_block_tally = touch_ends(jax.random.randint(splits[9], (N_FACE, N_TILE), 3, 5), jax.random.fold_in(splits[9], 1), 3, 4).astype(jnp.int32)
    return dict(airflow_components=airflow_components, heat_state=heat_state, layer_pressure_depth=layer_pressure_depth, constituent_masses=constituent_masses, ground_gravity_potential=ground_gravity_potential, inverse_mapping_entries=inverse_mapping_entries, mapping_determinant=mapping_determinant, interface_rightangle_rotations=interface_rightangle_rotations, interface_flipped_markers=interface_flipped_markers, corner_block_tally=corner_block_tally)


time_step = 0.05
viscosity = 0.05
highest = lax.Precision.HIGHEST

def gll_tables():
    offset = 1.0 / math.sqrt(5.0)
    gll_nodes = np.array([-1.0, -offset, offset, 1.0])
    weights = np.array([1.0 / 6.0, 5.0 / 6.0, 5.0 / 6.0, 1.0 / 6.0])
    barycentric = np.ones(4)
    for outer_index in range(4):
        for inner_index in range(4):
            if inner_index != outer_index:
                barycentric[outer_index] = barycentric[outer_index] / (gll_nodes[outer_index] - gll_nodes[inner_index])
    derivative = np.zeros((4, 4))
    for outer_index in range(4):
        for inner_index in range(4):
            if inner_index != outer_index:
                derivative[outer_index, inner_index] = barycentric[inner_index] / barycentric[outer_index] / (gll_nodes[outer_index] - gll_nodes[inner_index])
        derivative[outer_index, outer_index] = -np.sum(derivative[outer_index])
    return (derivative, weights)

def advance(east_wind, north_wind, temp_field, thick_field, tracer_field, geo_field, inverse_mapping_entries, mapping_determinant, along_rows, along_columns):

    def gradient(scalar):
        first_part = along_rows(scalar)
        second_part = along_columns(scalar)
        return (inverse_mapping_entries[0] * first_part + inverse_mapping_entries[2] * second_part, inverse_mapping_entries[1] * first_part + inverse_mapping_entries[3] * second_part)

    def divergence(east_part, north_part):
        first_flux = mapping_determinant * (inverse_mapping_entries[0] * east_part + inverse_mapping_entries[1] * north_part)
        second_flux = mapping_determinant * (inverse_mapping_entries[2] * east_part + inverse_mapping_entries[3] * north_part)
        return (along_rows(first_flux) + along_columns(second_flux)) / mapping_determinant
    energy = 0.5 * (east_wind * east_wind + north_wind * north_wind) + geo_field
    energy_x, energy_y = gradient(energy)
    temp_x, temp_y = gradient(temp_field)
    thick_x, thick_y = gradient(thick_field)
    laplace = divergence(thick_x, thick_y)
    new_east = east_wind - time_step * energy_x
    new_north = north_wind - time_step * energy_y
    new_temp = temp_field - time_step * (east_wind * temp_x + north_wind * temp_y)
    new_thick = thick_field - time_step * divergence(thick_field * east_wind, thick_field * north_wind) + time_step * viscosity * laplace
    new_tracer = tracer_field - time_step * divergence(tracer_field * east_wind, tracer_field * north_wind)
    spacing = jnp.sqrt(inverse_mapping_entries[0] * inverse_mapping_entries[0] + inverse_mapping_entries[1] * inverse_mapping_entries[1] + inverse_mapping_entries[2] * inverse_mapping_entries[2] + inverse_mapping_entries[3] * inverse_mapping_entries[3])
    courant = jnp.max(time_step * jnp.sqrt(east_wind * east_wind + north_wind * north_wind) * spacing)
    damping = jnp.max(time_step * viscosity * jnp.abs(laplace))
    fields = jnp.concatenate([new_east[None], new_north[None], new_temp[None], new_thick[None], new_tracer], 0)
    return (fields, courant, damping)

def turn(pieces, code):
    cosine = jnp.where(code == 0, 1.0, jnp.where(code == 2, -1.0, 0.0)).astype(jnp.float32)
    sine = jnp.where(code == 1, 1.0, jnp.where(code == 3, -1.0, 0.0)).astype(jnp.float32)
    first_part = cosine * pieces[0] - sine * pieces[1]
    second_part = sine * pieces[0] + cosine * pieces[1]
    return jnp.concatenate([first_part[None], second_part[None], pieces[2:]], 0)

def flip_edge(strip, flag):
    return jnp.where(flag[..., None] == 1, strip[..., ::-1], strip)

def fix_edge(strip, flag, code):
    return turn(flip_edge(strip, flag), code[..., None])

def assemble(inner, top_rim, bottom_rim, left_rim, right_rim, corner_ll, corner_lh, corner_hl, corner_hh):
    first_row = jnp.concatenate([corner_ll[..., None], top_rim, corner_lh[..., None]], -1)
    last_row = jnp.concatenate([corner_hl[..., None], bottom_rim, corner_hh[..., None]], -1)
    middle = jnp.concatenate([left_rim[..., None], inner, right_rim[..., None]], -1)
    return jnp.concatenate([first_row[..., None, :], middle, last_row[..., None, :]], -2)

def shared_sums(padded):
    row_count = padded.shape[-2] - 2
    column_count = padded.shape[-1] - 2
    row_low = (jnp.arange(row_count) % 4 == 0)[:, None]
    row_high = (jnp.arange(row_count) % 4 == 3)[:, None]
    across = padded[..., 1:-1, :] + jnp.where(row_low, padded[..., :-2, :], 0.0) + jnp.where(row_high, padded[..., 2:, :], 0.0)
    column_low = jnp.arange(column_count) % 4 == 0
    column_high = jnp.arange(column_count) % 4 == 3
    return across[..., 1:-1] + jnp.where(column_low, across[..., :-2], 0.0) + jnp.where(column_high, across[..., 2:], 0.0)

def combine_block(pieces, mass_pieces, rotations, flips, valences):
    inner, top_rim, bottom_rim, left_rim, right_rim, corner_ll, corner_lh, corner_hl, corner_hh = pieces
    mass_inner, mass_top, mass_bottom, mass_left, mass_right, mass_ll, mass_lh, mass_hl, mass_hh = mass_pieces
    top_code, bottom_code, left_code, right_code = rotations
    top_flag, bottom_flag, left_flag, right_flag = flips
    valence_ll, valence_lh, valence_hl, valence_hh = valences
    fixed = assemble(inner, fix_edge(top_rim, top_flag, top_code), fix_edge(bottom_rim, bottom_flag, bottom_code), fix_edge(left_rim, left_flag, left_code), fix_edge(right_rim, right_flag, right_code), jnp.where(valence_ll == 4, turn(corner_ll, (top_code + left_code) % 4), 0.0), jnp.where(valence_lh == 4, turn(corner_lh, (top_code + right_code) % 4), 0.0), jnp.where(valence_hl == 4, turn(corner_hl, (bottom_code + left_code) % 4), 0.0), jnp.where(valence_hh == 4, turn(corner_hh, (bottom_code + right_code) % 4), 0.0))
    mass_fixed = assemble(mass_inner, flip_edge(mass_top, top_flag), flip_edge(mass_bottom, bottom_flag), flip_edge(mass_left, left_flag), flip_edge(mass_right, right_flag), jnp.where(valence_ll == 4, mass_ll, 0.0), jnp.where(valence_lh == 4, mass_lh, 0.0), jnp.where(valence_hl == 4, mass_hl, 0.0), jnp.where(valence_hh == 4, mass_hh, 0.0))
    return shared_sums(fixed) / shared_sums(mass_fixed)

def block_pieces(field, face_count, tile_count):
    field_count = field.shape[0]
    row_count = field.shape[1] // face_count
    column_count = field.shape[2] // tile_count
    blocks = field.reshape(field_count, face_count, row_count, tile_count, column_count).transpose(0, 1, 3, 2, 4)
    top_rim = jnp.roll(blocks[:, :, :, -1, :], 1, axis=1)
    bottom_rim = jnp.roll(blocks[:, :, :, 0, :], -1, axis=1)
    left_rim = jnp.roll(blocks[:, :, :, :, -1], 1, axis=2)
    right_rim = jnp.roll(blocks[:, :, :, :, 0], -1, axis=2)
    corner_ll = jnp.roll(jnp.roll(blocks[:, :, :, -1, -1], 1, axis=1), 1, axis=2)
    corner_lh = jnp.roll(jnp.roll(blocks[:, :, :, -1, 0], 1, axis=1), -1, axis=2)
    corner_hl = jnp.roll(jnp.roll(blocks[:, :, :, 0, -1], -1, axis=1), 1, axis=2)
    corner_hh = jnp.roll(jnp.roll(blocks[:, :, :, 0, 0], -1, axis=1), -1, axis=2)
    return (blocks, top_rim, bottom_rim, left_rim, right_rim, corner_ll, corner_lh, corner_hl, corner_hh)

def reference(airflow_components, heat_state, layer_pressure_depth, constituent_masses, ground_gravity_potential, inverse_mapping_entries, mapping_determinant, interface_rightangle_rotations, interface_flipped_markers, corner_block_tally):
    derivative, weights = gll_tables()
    deriv_table = jnp.asarray(derivative, jnp.float32)

    def along_rows(field):
        field_shape = field.shape
        blocks = field.reshape(field_shape[:-2] + (field_shape[-2] // 4, 4, field_shape[-1]))
        return jnp.einsum('ab,...ebc->...eac', deriv_table, blocks, precision=highest).reshape(field_shape)

    def along_columns(field):
        field_shape = field.shape
        blocks = field.reshape(field_shape[:-1] + (field_shape[-1] // 4, 4))
        return jnp.einsum('ab,...eb->...ea', deriv_table, blocks, precision=highest).reshape(field_shape)
    strip_parts_sequence = heat_state * layer_pressure_depth
    column_total = lax.optimization_barrier(jnp.sum(strip_parts_sequence, axis=0))
    gravity_potential_altitude = ground_gravity_potential + (column_total - jnp.cumsum(strip_parts_sequence, axis=0)) + 0.5 * strip_parts_sequence
    grid_rows = mapping_determinant.shape[0]
    grid_columns = mapping_determinant.shape[1]
    weight_rows = jnp.asarray(np.tile(weights, grid_rows // 4), jnp.float32)
    weight_columns = jnp.asarray(np.tile(weights, grid_columns // 4), jnp.float32)
    mass = mapping_determinant * weight_rows[:, None] * weight_columns[None, :]
    turns_rows = interface_rightangle_rotations[:, :, 0]
    turns_columns = interface_rightangle_rotations[:, :, 1]
    rotations = ((4 - jnp.roll(turns_rows, 1, axis=0)) % 4, turns_rows, (4 - jnp.roll(turns_columns, 1, axis=1)) % 4, turns_columns)
    flips = (jnp.roll(interface_flipped_markers[:, :, 0], 1, axis=0), interface_flipped_markers[:, :, 0], jnp.roll(interface_flipped_markers[:, :, 1], 1, axis=1), interface_flipped_markers[:, :, 1])
    valences = (jnp.roll(jnp.roll(corner_block_tally, 1, axis=0), 1, axis=1), jnp.roll(corner_block_tally, 1, axis=0), jnp.roll(corner_block_tally, 1, axis=1), corner_block_tally)
    mass_pieces = block_pieces(mass[None], N_FACE, N_TILE)

    def lone_layer(level_inputs):
        wind_pair, temp_level, thick_level, tracer_level, geo_level = level_inputs
        fields, courant, damping = advance(wind_pair[0], wind_pair[1], temp_level, thick_level, tracer_level, geo_level, inverse_mapping_entries, mapping_determinant, along_rows, along_columns)
        pieces = block_pieces(fields * mass, N_FACE, N_TILE)
        substep_outcome = combine_block(pieces, mass_pieces, rotations, flips, valences)
        field_count = substep_outcome.shape[0]
        return (substep_outcome.transpose(0, 1, 3, 2, 4).reshape(field_count, grid_rows, grid_columns), courant, damping)
    piled_layers, stepwise_advection_number_layerwise, hyperdiffusion_change_layerwise = lax.map(lone_layer, (jnp.moveaxis(airflow_components, 1, 0), heat_state, layer_pressure_depth, jnp.moveaxis(constituent_masses, 1, 0), gravity_potential_altitude))
    airflow_next = jnp.moveaxis(piled_layers[:, 0:2], 0, 1)
    heat_state_next = piled_layers[:, 2]
    pressure_depth_next = piled_layers[:, 3]
    constituent_masses_next = jnp.moveaxis(piled_layers[:, 4:], 0, 1)
    stepping_bounds = jnp.stack([jnp.max(stepwise_advection_number_layerwise), jnp.max(hyperdiffusion_change_layerwise)])
    return (airflow_next, heat_state_next, pressure_depth_next, constituent_masses_next, stepping_bounds)
```

```python
import functools
import math

import jax
import jax.numpy as jnp
import numpy as np
from jax import lax
from jax.experimental import pallas as pl
from jax.experimental.pallas import tpu as pltpu
from jax.sharding import PartitionSpec as P

time_step = 0.05
viscosity = 0.05
f32 = jnp.float32
bf16 = jnp.bfloat16
MESH = pl.DeviceIdType.MESH
highest = lax.Precision.HIGHEST


def gll_tables():
    offset = 1.0 / math.sqrt(5.0)
    nodes = np.array([-1.0, -offset, offset, 1.0])
    weights = np.array([1.0 / 6.0, 5.0 / 6.0, 5.0 / 6.0, 1.0 / 6.0])
    bary = np.ones(4)
    for i in range(4):
        for j in range(4):
            if j != i:
                bary[i] = bary[i] / (nodes[i] - nodes[j])
    derivative = np.zeros((4, 4))
    for i in range(4):
        for j in range(4):
            if j != i:
                derivative[i, j] = bary[j] / bary[i] / (nodes[i] - nodes[j])
        derivative[i, i] = -np.sum(derivative[i])
    return derivative, weights


def lane_tables(columns):
    derivative, weights = gll_tables()
    d = np.kron(np.eye(columns // 4), derivative)
    s = np.eye(columns)
    for c in range(columns - 1):
        if c % 4 == 3:
            s[c, c + 1] = s[c + 1, c] = 1.0
    w = np.tile(weights, columns // 4)
    t = (-time_step * (d.T * w[None, :]) @ s).astype(np.float32)
    t_hi = jnp.asarray(t).astype(bf16)
    t_lo = (jnp.asarray(t) - t_hi.astype(f32)).astype(bf16)
    sb = jnp.asarray(s, bf16)
    d_t = jnp.asarray(d.T, f32)
    d_hi = d_t.astype(bf16)
    d_lo = (d_t - d_hi.astype(f32)).astype(bf16)
    return jnp.concatenate([sb, sb, t_hi, t_hi, t_lo], 0), jnp.concatenate([d_hi, d_hi, d_lo], 0), jnp.asarray(w[None, :], f32)


def split(x):
    hi = x.astype(bf16)
    return hi, (x - hi.astype(f32)).astype(bf16)


def layout(levels, tracers):
    group = 8 // math.gcd(levels, 8)
    chunks, q = [], 0
    while q < tracers:
        n = min(group, tracers - q)
        chunks.append((q * levels, -(-n * levels // 8) * 8, n * levels))
        q += n
    return chunks


def packing(levels, chunks):
    out = [(0, 1, 1)]
    for tiles in [c[1] // 8 for c in chunks] + [2 * (levels // 8) + 1] * 2:
        quads = (tiles - 1) // 4
        out.append((quads, tiles - quads, 8 * (tiles - quads)))
    return out


def kernel(
    sizes, dims,
    wind_h, temp_h, thick_h, tracer_h, ground_h, maps_h, det_h, ops_h, dct_h, wc_h,
    rot_h, flip_h, tally_h,
    wind_o, temp_o, thick_o, tracer_o, bound_o,
    wind, temp, thick, tracer, geo, ground, maps, det, ops, dct, wc,
    a_ref, b_ref, z_ref, below, above_ref, pack, corner, total, peak,
    up_in, down_in, left_in, right_in, corner_in, total_in, peak_in,
    rot_ref, flip_ref, tally_ref,
    in_sem, sent_sem, piece_sem, corner_sem, total_sem, peak_sem,
):
    nf, nt, nl = sizes
    levels, rows, columns, chunks, pad = dims
    derivative, weights = gll_tables()
    rep = [a - (a // 4) for a in range(rows)]
    distinct = rows - rows // 4 + 1
    face, tile, lev = lax.axis_index("face"), lax.axis_index("tile"), lax.axis_index("lev")
    f_up, f_dn = lax.rem(face + nf - 1, nf), lax.rem(face + 1, nf)
    t_lf, t_rt = lax.rem(tile + nt - 1, nt), lax.rem(tile + 1, nt)

    pieces = [(0, 8, 1)]
    at = 8
    for _, count, _ in chunks:
        pieces.append((at, count, 1))
        at += count
    pieces.append((at, 2 * pad, 1))
    pieces.append((at + 2 * pad, 2 * pad, 2))
    first_pack = np.cumsum([0] + [p[2] for p in pieces]).tolist()
    last = len(pieces) - 1
    heat = last - 1
    full, tail = levels // 8, levels % 8
    packed = packing(levels, chunks)
    first_row = np.cumsum([0] + [8 * p[1] for p in packed]).tolist()
    quarter = columns // 4
    side_rows = [1] + [8 * p[2] for p in pieces[1:]]

    n = levels * rows
    groups_in = [
        [(maps_h, maps), (det_h, det), (wc_h, wc),
         (wind_h.at[0], wind.at[0, :n]), (wind_h.at[1], wind.at[1, :n])],
        [(temp_h, temp.at[:n]), (thick_h, thick.at[:n])],
        [(ops_h, ops)],
        [(dct_h, dct), (ground_h, ground)],
    ]
    group_rows = [5 * rows + 1 + 2 * n, 2 * n, 5 * columns // 2, 3 * columns // 2 + rows]
    n0 = len(groups_in)
    spans = [pl.ds(start * rows, valid * rows) for start, _, valid in chunks]
    traced = [
        pltpu.make_async_copy(tracer_h.at[span], tracer.at[span], in_sem.at[n0 + k])
        for k, span in enumerate(spans)
    ]
    tables = [(rot_h, rot_ref), (flip_h, flip_ref), (tally_h, tally_ref)]
    at = n0 + len(chunks)
    tables = [pltpu.make_async_copy(s, d, in_sem.at[at + i]) for i, (s, d) in enumerate(tables)]

    def fetch(i):
        for s, d in groups_in[i]:
            pltpu.make_async_copy(s, d, in_sem.at[i]).start()

    def drain(count, sem):
        view = z_ref.at[0, pl.ds(0, count)] if count <= z_ref.shape[1] else tracer.at[pl.ds(0, count)]
        pltpu.make_async_copy(view, view, sem).wait()

    fetch(0)
    traced[0].start()
    fetch(2)
    fetch(1)
    for load in traced[1:]:
        load.start()
    fetch(3)
    for load in tables:
        load.start()

    peers = [(lax.rem(face + o, nf), tile, lev) for o in range(1, nf)]
    peers += [(face, lax.rem(tile + o, nt), lev) for o in range(1, nt)]
    peers += [(face, tile, lax.rem(lev + o, nl)) for o in range(1, nl)]
    diagonals = [(f_dn, t_rt, lev), (f_dn, t_lf, lev), (f_up, t_rt, lev), (f_up, t_lf, lev)]
    barrier = pltpu.get_barrier_semaphore()
    for peer in peers + diagonals:
        pl.semaphore_signal(barrier, inc=1, device_id=peer, device_id_type=MESH)

    extra = (pad - levels) * rows
    if extra:
        zero = jnp.zeros((extra, columns), f32)
        temp[levels * rows :, :] = zero
        thick[levels * rows :, :] = zero
        geo[levels * rows :, :] = zero
        wind[0, levels * rows :, :] = zero
        wind[1, levels * rows :, :] = zero
    end = chunks[-1][0] + chunks[-1][2]
    more = chunks[-1][1] - chunks[-1][2]
    if more:
        tracer[end * rows :, :] = jnp.zeros((more * rows, columns), f32)

    sent = []

    def send(src, dst, r, to):
        pltpu.make_async_remote_copy(
            src_ref=src, dst_ref=dst, send_sem=sent_sem.at[0], recv_sem=r,
            device_id=to, device_id_type=MESH,
        ).start()
        sent.append(math.prod(src.shape) // columns)

    def column_sums():
        drain(group_rows[1], in_sem.at[1])
        acc = jnp.zeros((rows, columns), f32)
        for k in reversed(range(levels)):
            term = temp[k * rows : (k + 1) * rows, :] * thick[k * rows : (k + 1) * rows, :]
            geo[k * rows : (k + 1) * rows, :] = acc + 0.5 * term
            acc = acc + term
        total[...] = acc
        for o in range(1, nl):
            send(total, total_in.at[o - 1], total_sem.at[0], (face, tile, lax.rem(lev + o, nl)))

    drain(group_rows[0], in_sem.at[0])
    w_col = wc[...]
    drain(group_rows[2], in_sem.at[2])
    table = ops[...]
    narrow = ops[: 2 * columns, :]
    wr = [float(weights[a % 4]) for a in range(rows)]
    m = [[maps[e * rows + a : e * rows + a + 1, :] for a in range(rows)] for e in range(4)]
    jac = [det[a : a + 1, :] for a in range(rows)]
    mass = [jac[a] * (wr[a] * w_col) for a in range(rows)]
    step_d = [[float(time_step * wr[a] * derivative[a % 4, b]) for b in range(4)] for a in range(rows)]
    dd = [[float(derivative[i, j]) for j in range(4)] for i in range(4)]

    def level_rows(ref, a):
        return ref[pl.ds(a, pad, stride=rows), :]

    def along_rows(values, a, coef):
        base = a - a % 4
        out = coef[0] * values[base]
        for b in range(1, 4):
            out = out + coef[b] * values[base + b]
        return out

    def merged(values):
        out = [None] * distinct
        for a in range(rows):
            r = rep[a]
            out[r] = values[a] if out[r] is None else out[r] + values[a]
        return out

    def lanes_plain(x):
        hi, lo = split(x)
        return jnp.dot(jnp.concatenate([hi, lo], 1), narrow, preferred_element_type=f32)

    def lanes_both(p, g):
        ph, plo = split(p)
        gh, glo = split(g)
        return jnp.dot(
            jnp.concatenate([ph, plo, gh, glo, gh], 1), table, preferred_element_type=f32
        )

    def by_column(values):
        stacked = jnp.concatenate(values, 0)
        hi, lo = split(stacked)
        out = jnp.dot(
            jnp.concatenate([hi, lo, hi], 1), dct[...], preferred_element_type=f32
        )
        n = values[0].shape[0]
        return [out[i * n : (i + 1) * n] for i in range(len(values))]

    lane = lax.broadcasted_iota(jnp.int32, (8, columns), 1)
    unit = 2 * distinct
    within = lax.rem(lane, unit)

    def put(piece, offset, r, z):
        z_ref[r, piece + offset : piece + offset + z.shape[0], :] = z

    def pack_of(start, groups):
        out = jnp.zeros((8, columns), f32)
        for i in range(groups):
            for r in range(distinct):
                spot = unit * i + 2 * r
                value = pltpu.roll(z_ref[r, start + 8 * i : start + 8 * i + 8, :], spot + 1, 1)
                out = jnp.where((lane == spot) | (lane == spot + 1), value, out)
        return out

    squeeze = jnp.minimum(lane + lane // 3, columns - 1)
    sublane = lax.broadcasted_iota(jnp.int32, (8, columns), 0)

    def tiles_of(j, r):
        start, count, _ = pieces[j]

        def tile_at(row):
            return z_ref[r, row : row + 8, :]

        if j < heat:
            return [tile_at(start + 8 * i) for i in range(count // 8)]
        out = [tile_at(start + half + 8 * i) for half in (0, pad) for i in range(full)]
        second = pltpu.roll(tile_at(start + pad + 8 * full), tail, 0)
        return out + [jnp.where(sublane < tail, tile_at(start + 8 * full), second)]

    def ship_rows(j):
        quads, width, height = packed[j]
        if j == 0:
            send(z_ref.at[distinct - 1, pl.ds(0, 1)], up_in.at[pl.ds(0, 1)], piece_sem.at[0], (f_dn, tile, lev))
            send(z_ref.at[0, pl.ds(0, 1)], down_in.at[pl.ds(0, 1)], piece_sem.at[0], (f_up, tile, lev))
            return
        at = first_row[j]
        for r, out, landing, to in (
            (distinct - 1, below, up_in, (f_dn, tile, lev)), (0, above_ref, down_in, (f_up, tile, lev))
        ):
            wide = tiles_of(j, r)
            thin = [jnp.take_along_axis(x, squeeze, axis=1) for x in wide]
            done = []
            for g in range(quads):
                spare = thin[4 * g + 3]
                for t in range(3):
                    done.append(jnp.where(
                        lane < 3 * quarter, thin[4 * g + t],
                        pltpu.roll(spare, (3 - t) * quarter, 1),
                    ))
            done += thin[4 * quads :]
            for i in range(4 * quads):
                spot = 3 * quarter + 1 + i
                done[-1] = jnp.where(
                    lane == spot, pltpu.roll(wide[i], (spot + 1) % columns, 1), done[-1]
                )
            for i, x in enumerate(done):
                out[at + 8 * i : at + 8 * i + 8, :] = x
            span = pl.ds(at, height)
            send(out.at[span], landing.at[span], piece_sem.at[j], to)

    def ship_sides(j):
        start, count, packs = pieces[j]
        each = count // packs
        made = []
        for p in range(packs):
            made.append(pack_of(start + p * each, each // 8))
            pack[first_pack[j] + p] = made[-1]
        span = pl.ds(first_pack[j], packs)
        for landing, to in ((left_in, (face, t_rt, lev)), (right_in, (face, t_lf, lev))):
            if j == 0:
                send(pack.at[0, pl.ds(0, 1)], landing.at[0, pl.ds(0, 1)], piece_sem.at[0], to)
            else:
                send(pack.at[span], landing.at[span], piece_sem.at[j], to)
        return made

    source = [unit - 2, unit - 1, 0, 1]

    def ship_corners(which, made):
        for d in range(4):
            out = jnp.zeros((8, columns), f32)
            for p, value in enumerate(made):
                out = jnp.where(within == p, pltpu.roll(value, (p - source[d]) % columns, 1), out)
            corner[which, d] = out
            part = pl.ds(0, 8 if which else 1)
            send(corner.at[which, d, part], corner_in.at[which, d, part],
                 corner_sem.at[which], diagonals[d])

    east = [level_rows(wind.at[0], a) for a in range(rows)]
    north = [level_rows(wind.at[1], a) for a in range(rows)]
    speed, parts = None, []
    whole = max(c[1] for c in chunks)
    for a in range(rows):
        aa = jac[a] * (m[0][a] * east[a] + m[1][a] * north[a])
        bb = jac[a] * (m[2][a] * east[a] + m[3][a] * north[a])
        parts.append(((aa * w_col)[:levels], (bb * wr[a])[:levels]))
        spacing = jnp.sqrt(
            m[0][a] * m[0][a] + m[1][a] * m[1][a] + m[2][a] * m[2][a] + m[3][a] * m[3][a]
        )
        here = jnp.max(east[a] * east[a] + north[a] * north[a], axis=0, keepdims=True)
        here = jnp.sqrt(here) * spacing
        speed = here if speed is None else jnp.maximum(speed, here)

    @pl.when(face < nf)
    def _():
        for a, pair in enumerate(parts):
            for k in range(-(-whole // levels)):
                n = min(levels, whole - k * levels)
                a_ref[a, k * levels : k * levels + n, :] = pair[0][:n]
                b_ref[a, k * levels : k * levels + n, :] = pair[1][:n]

    def tracers_of(k):
        start, count, _ = chunks[k]
        traced[k].wait()
        q = [tracer[pl.ds(start * rows + a, count, stride=rows), :] for a in range(rows)]
        first = [q[a] * a_ref[a, :count, :] for a in range(rows)]
        keep = [mass[a] * q[a] - along_rows(first, a, step_d[a]) for a in range(rows)]
        second = [q[a] * b_ref[a, :count, :] for a in range(rows)]
        for r, (x, y) in enumerate(zip(merged(keep), merged(second))):
            put(pieces[k + 1][0], 0, r, lanes_both(x, y))

    def tracers_ship(k):
        ship_rows(k + 1)
        return ship_sides(k + 1)

    tracers_of(0)
    pl.semaphore_wait(barrier, len(peers) + len(diagonals))
    made = tracers_ship(0)
    column_sums()
    for r, x in enumerate(merged(mass)):
        put(0, 0, r, lanes_plain(jnp.broadcast_to(x, (8, columns))))
    ship_rows(0)
    ship_corners(0, ship_sides(0))
    drain(group_rows[3], in_sem.at[3])
    depth = [level_rows(thick, a) for a in range(rows)]
    depth_c = by_column(depth)
    flux_a, flux_b = [], []
    for a in range(rows):
        dr, dc = along_rows(depth, a, dd[a % 4]), depth_c[a]
        gx, gy = m[0][a] * dr + m[2][a] * dc, m[1][a] * dr + m[3][a] * dc
        flux_a.append(jac[a] * (m[0][a] * gx + m[1][a] * gy))
        flux_b.append(jac[a] * (m[2][a] * gx + m[3][a] * gy))
    flux_c = by_column(flux_b)
    damp = None
    for a in range(rows):
        lap = jnp.abs(along_rows(flux_a, a, dd[a % 4]) + flux_c[a])
        here = jnp.max(lap, axis=0, keepdims=True) / jac[a]
        damp = here if damp is None else jnp.maximum(damp, here)
    peak[0] = jnp.concatenate(
        [time_step * speed, (time_step * viscosity) * damp, jnp.zeros((6, columns), f32)], 0
    )
    for o in range(1, nf):
        send(peak.at[0], peak_in.at[o - 1], peak_sem.at[0], (lax.rem(face + o, nf), tile, lev))

    early = min(3, len(chunks))
    for k in range(1, early):
        tracers_of(k)
        made += tracers_ship(k)

    first, second, keep = [], [], []
    for a in range(rows):
        aa = jac[a] * (m[0][a] * east[a] + m[1][a] * north[a])
        bb = jac[a] * (m[2][a] * east[a] + m[3][a] * north[a])
        first.append(w_col * (depth[a] * aa - viscosity * flux_a[a]))
        second.append(wr[a] * (depth[a] * bb - viscosity * flux_b[a]))
    for a in range(rows):
        keep.append(mass[a] * depth[a] - along_rows(first, a, step_d[a]))
    for r, (x, y) in enumerate(zip(merged(keep), merged(second))):
        put(pieces[heat][0], pad, r, lanes_both(x, y))
    warm = [level_rows(temp, a) for a in range(rows)]
    warm_c = by_column(warm)
    value = []
    for a in range(rows):
        dr, dc = along_rows(warm, a, dd[a % 4]), warm_c[a]
        gx, gy = m[0][a] * dr + m[2][a] * dc, m[1][a] * dr + m[3][a] * dc
        value.append(mass[a] * (warm[a] - time_step * (east[a] * gx + north[a] * gy)))
    for r, x in enumerate(merged(value)):
        put(pieces[heat][0], 0, r, lanes_plain(x))
    dynamic = ship_sides(heat)

    for k in range(early, len(chunks)):
        tracers_of(k)
        made += ship_sides(k + 1)
    ship_corners(1, made)

    above = ground[...]
    if nl > 1:
        drain((nl - 1) * rows, total_sem.at[0])
    for o in range(nl - 1):
        origin = lax.rem(lev + nl - (o + 1), nl)
        use = jnp.where(origin > lev, 1.0, 0.0).astype(f32)
        above = above + use * total_in[o]
    energy = []
    for a in range(rows):
        u, v = level_rows(wind.at[0], a), level_rows(wind.at[1], a)
        energy.append(0.5 * (u * u + v * v) + level_rows(geo, a) + above[a : a + 1, :])
    energy_c = by_column(energy)
    value_u, value_v = [], []
    for a in range(rows):
        u, v = level_rows(wind.at[0], a), level_rows(wind.at[1], a)
        dr, dc = along_rows(energy, a, dd[a % 4]), energy_c[a]
        value_u.append(mass[a] * (u - time_step * (m[0][a] * dr + m[2][a] * dc)))
        value_v.append(mass[a] * (v - time_step * (m[1][a] * dr + m[3][a] * dc)))
    for r, (x, y) in enumerate(zip(merged(value_u), merged(value_v))):
        put(pieces[last][0], 0, r, lanes_plain(x))
        put(pieces[last][0], pad, r, lanes_plain(y))
    dynamic += ship_sides(last)
    ship_corners(2, dynamic)
    ship_rows(last)
    for k in range(early, len(chunks)):
        ship_rows(k + 1)
    ship_rows(heat)

    def gathered(stage, base, count):
        best = peak[stage]
        if count:
            drain(8 * count, peak_sem.at[stage])
        for o in range(count):
            best = jnp.maximum(best, peak_in[base + o])
        return best

    def second_stage():
        peak[1] = gathered(0, 0, nf - 1)
        base = nf - 1
        for o in range(1, nt):
            send(peak.at[1], peak_in.at[base + o - 1], peak_sem.at[1],
                 (face, lax.rem(tile + o, nt), lev))

    def third_stage():
        peak[2] = gathered(1, nf - 1, nt - 1)
        base = nf + nt - 2
        for o in range(1, nl):
            send(peak.at[2], peak_in.at[base + o - 1], peak_sem.at[2],
                 (face, tile, lax.rem(lev + o, nl)))

    for load in tables:
        load.wait()

    def seam(ref, f, t, k):
        return ref[f, k, t]

    codes = [
        lax.rem(4 - seam(rot_ref, f_up, tile, 0), 4), seam(rot_ref, face, tile, 0),
        lax.rem(4 - seam(rot_ref, face, t_lf, 1), 4), seam(rot_ref, face, tile, 1),
    ]
    flips = [
        seam(flip_ref, f_up, tile, 0), seam(flip_ref, face, tile, 0),
        seam(flip_ref, face, t_lf, 1), seam(flip_ref, face, tile, 1),
    ]
    tallies = [
        tally_ref[f_up, t_lf], tally_ref[f_up, tile],
        tally_ref[face, t_lf], tally_ref[face, tile],
    ]

    def cosine(code):
        return jnp.where(code == 0, 1.0, jnp.where(code == 2, -1.0, 0.0)).astype(f32)

    def sine(code):
        return jnp.where(code == 1, 1.0, jnp.where(code == 3, -1.0, 0.0)).astype(f32)

    def filled(x):
        return jnp.full((8, columns), x)

    odd = lax.rem(lane, 2) == 1
    mirror = lane - within + (unit - 2) - 2 * (within // 2) + lax.rem(within, 2)
    mirror = jnp.clip(mirror, 0, columns - 1)
    side_flip = jnp.where(odd, filled(flips[2]), filled(flips[3])) == 1
    side_cos = jnp.where(odd, filled(cosine(codes[2])), filled(cosine(codes[3])))
    side_sin = jnp.where(odd, filled(sine(codes[2])), filled(sine(codes[3])))
    corner_code = [
        lax.rem(codes[0] + codes[2], 4), lax.rem(codes[0] + codes[3], 4),
        lax.rem(codes[1] + codes[2], 4), lax.rem(codes[1] + codes[3], 4),
    ]
    target = [1, 0, unit - 1, unit - 2]
    alive = [filled(tallies[d]) == 4 for d in range(4)]

    def sides(index):
        if index == 0:
            a = jnp.broadcast_to(left_in[0, 0:1, :], (8, columns))
            b = jnp.broadcast_to(right_in[0, 0:1, :], (8, columns))
        else:
            a, b = left_in[index], right_in[index]
        x = jnp.where(odd, pltpu.roll(a, 1, 1), pltpu.roll(b, columns - 1, 1))
        return jnp.where(side_flip, jnp.take_along_axis(x, mirror, axis=1), x)

    def corner_values(which, d, p):
        x = corner_in[which, d] if which else jnp.broadcast_to(corner_in[0, d, 0:1, :], (8, columns))
        x = pltpu.roll(x, (target[d] - p) % columns, 1)
        return jnp.where(alive[d] & (within == target[d]), x, 0.0)

    groups = pad // 8
    edge = (lane[:1] == 0) | (lane[:1] == columns - 1)

    def to_edges(x, i, r):
        y = pltpu.roll(x, (columns - (unit * i + 2 * r + 1)) % columns, 1)
        return jnp.where(edge, y, 0.0)

    rev = (columns - 1) - lane
    row_flip = [filled(flips[0]) == 1, filled(flips[1]) == 1]
    origin_lane = [jnp.where(row_flip[i], rev, lane) for i in range(2)]
    spread = [x - x // 4 for x in origin_lane]
    inner = [jnp.minimum(x, 3 * quarter - 1) for x in spread]
    rim_end = [x == columns - 1 for x in origin_lane]

    def row_rim(ref, which, j):
        if j == 0:
            x = jnp.broadcast_to(ref[0:1, :], (8, columns))
            return [jnp.take_along_axis(x, origin_lane[which], axis=1)]
        quads, width, _ = packed[j]
        at = first_row[j]
        got = [ref[at + 8 * i : at + 8 * i + 8, :] for i in range(width)]
        ends = got[-1]
        out = []
        for g in range(quads):
            one, two, three = got[3 * g : 3 * g + 3]
            four = jnp.where(
                lane < quarter, pltpu.roll(one, quarter, 1),
                jnp.where(lane < 2 * quarter, pltpu.roll(two, 2 * quarter, 1),
                          pltpu.roll(three, 3 * quarter, 1)),
            )
            for x in (one, two, three, four):
                spot = 3 * quarter + 1 + len(out)
                x = jnp.take_along_axis(x, inner[which], axis=1)
                end = jnp.broadcast_to(ends[:, spot : spot + 1], (8, columns))
                out.append(jnp.where(rim_end[which], end, x))
        for x in got[3 * quads :]:
            out.append(jnp.take_along_axis(x, spread[which], axis=1))
        if j >= heat:
            second = pltpu.roll(out[-1], 8 - tail, 0)
            out = out[:full] + out[-1:] + out[full : 2 * full] + [second]
        return out

    def arrived(j, corners=None):
        drain(2 * packed[j][2] + 2 * side_rows[j], piece_sem.at[j])
        if corners is not None:
            drain(4 * (8 if corners else 1), corner_sem.at[corners])

    def finished(start, i, r, side, i_side, top, bottom):
        x = z_ref[r, start + 8 * i : start + 8 * i + 8, :] + to_edges(side, i_side, r)
        if r == 0:
            x = x + top
        if r == distinct - 1:
            x = x + bottom
        return x

    def store(ref, begin, i, valid, r, x):
        n = min(8, valid - 8 * i)
        if n <= 0:
            return
        for a in range(rows):
            if rep[a] == r:
                ref[pl.ds((begin + 8 * i) * rows + a, n, stride=rows), :] = (x * inverse[a])[:n]

    arrived(0, 0)
    x = sides(0)
    for d in range(4):
        x = x + corner_values(0, d, 0)
    top, bottom = row_rim(up_in, 0, 0), row_rim(down_in, 1, 0)
    inverse = [None] * rows
    for r in range(distinct):
        whole_mass = 1.0 / finished(0, 0, r, x, 0, top[0], bottom[0])
        for a in range(rows):
            if rep[a] == r:
                inverse[a] = whole_mass

    def finish_tracers(k):
        start, count, valid = chunks[k]
        j = k + 1
        arrived(j, 1 if k == 0 else None)
        x = sides(first_pack[j])
        for d in range(4):
            x = x + corner_values(1, d, k)
        top = row_rim(up_in, 0, j)
        bottom = row_rim(down_in, 1, j)
        for i in range(count // 8):
            for r in range(distinct):
                store(tracer_o, start, i, valid, r,
                      finished(pieces[j][0], i, r, x, i, top[i], bottom[i]))

    second_stage()
    finish_tracers(0)
    for k in range(1, early):
        finish_tracers(k)
    third_stage()

    arrived(last, 2)
    p = first_pack[last]
    xu, xv = sides(p), sides(p + 1)
    xu, xv = side_cos * xu - side_sin * xv, side_sin * xu + side_cos * xv
    for d in range(4):
        cu, cv = corner_values(2, d, 1), corner_values(2, d, 2)
        c, s = cosine(corner_code[d]), sine(corner_code[d])
        xu, xv = xu + (c * cu - s * cv), xv + (s * cu + c * cv)
    begin = pieces[last][0]
    rims = []
    for which, ref in ((0, up_in), (1, down_in)):
        both = row_rim(ref, which, last)
        c, s = cosine(codes[which]), sine(codes[which])
        ru = [c * both[i] - s * both[groups + i] for i in range(groups)]
        rv = [s * both[i] + c * both[groups + i] for i in range(groups)]
        rims.append((ru, rv))
    for i in range(groups):
        for r in range(distinct):
            store(wind_o.at[0], 0, i, levels, r,
                  finished(begin, i, r, xu, i, rims[0][0][i], rims[1][0][i]))
            store(wind_o.at[1], 0, i, levels, r,
                  finished(begin + pad, i, r, xv, i, rims[0][1][i], rims[1][1][i]))

    for k in range(early, len(chunks)):
        finish_tracers(k)

    arrived(heat)
    begin = pieces[heat][0]
    x = sides(first_pack[heat])
    for d in range(4):
        x = x + corner_values(2, d, 0)
    top, bottom = row_rim(up_in, 0, heat), row_rim(down_in, 1, heat)
    for i in range(groups):
        for r in range(distinct):
            store(temp_o, 0, i, levels, r, finished(begin, i, r, x, i, top[i], bottom[i]))
            j = groups + i
            store(thick_o, 0, i, levels, r, finished(begin, j, r, x, j, top[j], bottom[j]))

    bound_o[...] = gathered(2, nf + nt - 2, nl - 1)
    drain(sum(sent), sent_sem.at[0])


def write_out(wind, temp, thick, tracer, bound, wind_o, temp_o, thick_o, tracer_o, bound_o, sem):
    pairs = ((tracer, tracer_o), (wind, wind_o), (temp, temp_o), (thick, thick_o))
    copies = [pltpu.make_async_copy(a, b, sem.at[i]) for i, (a, b) in enumerate(pairs)]
    for copy in copies:
        copy.start()
    bound_o[0] = jnp.max(bound[0:1, :])
    bound_o[1] = jnp.max(bound[1:2, :])
    for copy in copies:
        copy.wait()


def on_device(
    sizes, wind, temp, thick, tracers, ground, maps, det, rot, flip, tally
):
    nf, nt, nl = sizes
    levels, rows, columns = temp.shape
    if rows != 8 or columns != 128 or levels % 8 not in (1, 2, 3, 4):
        raise ValueError("block shape")
    count = tracers.shape[0]
    chunks = layout(levels, count)
    pad = -(-levels // 8) * 8
    table, dct, w_col = lane_tables(columns)
    distinct = rows - rows // 4 + 1
    total_rows = 4 * pad + 8 + sum(c[1] for c in chunks)
    pieces = len(chunks) + 3
    packs = len(chunks) + 4
    landing = sum(8 * p[1] for p in packing(levels, chunks))
    whole = max(c[1] for c in chunks)
    n = levels * rows
    dma = pltpu.SemaphoreType.DMA
    peers = nf + nt + nl - 3
    hbm = pl.BlockSpec(memory_space=pl.ANY)
    smem = pl.BlockSpec(memory_space=pltpu.SMEM)
    vmem = pl.BlockSpec(memory_space=pltpu.VMEM)
    last = chunks[-1]
    shapes = ((2, n, columns), (n, columns), (n, columns), (count * n, columns), (8, columns))
    outs = pl.pallas_call(
        functools.partial(kernel, sizes, (levels, rows, columns, chunks, pad)),
        out_shape=tuple(pltpu.VMEM(shape, f32) for shape in shapes),
        in_specs=[hbm] * 13,
        out_specs=(vmem,) * 5,
        scratch_shapes=[
            pltpu.VMEM((2, pad * rows, columns), f32),
            pltpu.VMEM((pad * rows, columns), f32),
            pltpu.VMEM((pad * rows, columns), f32),
            pltpu.VMEM(((last[0] + last[1]) * rows, columns), f32),
            pltpu.VMEM((pad * rows, columns), f32),
            pltpu.VMEM((rows, columns), f32),
            pltpu.VMEM((4 * rows, columns), f32),
            pltpu.VMEM((rows, columns), f32),
            pltpu.VMEM(table.shape, bf16),
            pltpu.VMEM(dct.shape, bf16),
            pltpu.VMEM((1, columns), f32),
            pltpu.VMEM((rows, whole, columns), f32),
            pltpu.VMEM((rows, whole, columns), f32),
            pltpu.VMEM((distinct, total_rows, columns), f32),
            pltpu.VMEM((landing, columns), f32),
            pltpu.VMEM((landing, columns), f32),
            pltpu.VMEM((packs, 8, columns), f32),
            pltpu.VMEM((3, 4, 8, columns), f32),
            pltpu.VMEM((rows, columns), f32),
            pltpu.VMEM((3, 8, columns), f32),
            pltpu.VMEM((landing, columns), f32),
            pltpu.VMEM((landing, columns), f32),
            pltpu.VMEM((packs, 8, columns), f32),
            pltpu.VMEM((packs, 8, columns), f32),
            pltpu.VMEM((3, 4, 8, columns), f32),
            pltpu.VMEM((nl - 1, rows, columns), f32),
            pltpu.VMEM((peers, 8, columns), f32),
            pltpu.SMEM((nf, 2, nt), jnp.int32),
            pltpu.SMEM((nf, 2, nt), jnp.int32),
            pltpu.SMEM((nf, nt), jnp.int32),
            dma((7 + len(chunks),)),
            dma((1,)),
            dma((pieces,)),
            dma((3,)),
            dma((1,)),
            dma((3,)),
        ],
        compiler_params=pltpu.CompilerParams(collective_id=0, has_side_effects=True),
    )(
        wind.reshape(2, n, columns), temp.reshape(n, columns), thick.reshape(n, columns),
        tracers.reshape(count * n, columns), ground, maps.reshape(4 * rows, columns), det,
        table, dct, w_col, rot.transpose(0, 2, 1), flip.transpose(0, 2, 1), tally,
    )
    outs = pl.pallas_call(
        write_out,
        out_shape=tuple(jax.ShapeDtypeStruct(x, f32) for x in shapes[:4] + ((2,),)),
        in_specs=[vmem] * 5,
        out_specs=(hbm,) * 4 + (smem,),
        scratch_shapes=[dma((4,))],
    )(*[pltpu.with_memory_space_constraint(x, pltpu.VMEM) for x in outs])
    return (
        outs[0].reshape(wind.shape), outs[1].reshape(temp.shape), outs[2].reshape(thick.shape),
        outs[3].reshape(tracers.shape), outs[4],
    )


def solution(mesh):
    sizes = tuple(mesh.shape[name] for name in ("face", "tile", "lev"))
    level = P("lev", "face", "tile")
    stacked = P(None, "lev", "face", "tile")
    return jax.shard_map(
        functools.partial(on_device, sizes),
        mesh=mesh,
        in_specs=(stacked, level, level, stacked, P("face", "tile"), P(None, "face", "tile"),
                  P("face", "tile"), P(), P(), P()),
        out_specs=(stacked, level, level, stacked, P()),
        check_vma=False,
    )
```

```python
import functools
import math

import jax
import jax.numpy as jnp
import numpy as np
from jax import lax
from jax.experimental import pallas as pl
from jax.experimental.pallas import tpu as pltpu
from jax.sharding import PartitionSpec as P

time_step = 0.05
viscosity = 0.05
f32 = jnp.float32
bf16 = jnp.bfloat16
MESH = pl.DeviceIdType.MESH
highest = lax.Precision.HIGHEST


def gll_tables():
    offset = 1.0 / math.sqrt(5.0)
    nodes = np.array([-1.0, -offset, offset, 1.0])
    weights = np.array([1.0 / 6.0, 5.0 / 6.0, 5.0 / 6.0, 1.0 / 6.0])
    bary = np.ones(4)
    for i in range(4):
        for j in range(4):
            if j != i:
                bary[i] = bary[i] / (nodes[i] - nodes[j])
    derivative = np.zeros((4, 4))
    for i in range(4):
        for j in range(4):
            if j != i:
                derivative[i, j] = bary[j] / bary[i] / (nodes[i] - nodes[j])
        derivative[i, i] = -np.sum(derivative[i])
    return derivative, weights


def lane_tables(columns):
    derivative, weights = gll_tables()
    d = np.kron(np.eye(columns // 4), derivative)
    s = np.eye(columns)
    for c in range(columns - 1):
        if c % 4 == 3:
            s[c, c + 1] = s[c + 1, c] = 1.0
    w = np.tile(weights, columns // 4)
    t = (-time_step * (d.T * w[None, :]) @ s).astype(np.float32)
    t_hi = jnp.asarray(t).astype(bf16)
    t_lo = (jnp.asarray(t) - t_hi.astype(f32)).astype(bf16)
    sb = jnp.asarray(s, bf16)
    d_t = jnp.asarray(d.T, f32)
    d_hi = d_t.astype(bf16)
    d_lo = (d_t - d_hi.astype(f32)).astype(bf16)
    return jnp.concatenate([sb, sb, t_hi, t_hi, t_lo], 0), jnp.concatenate([d_hi, d_hi, d_lo], 0), jnp.asarray(w[None, :], f32)


def split(x):
    hi = x.astype(bf16)
    return hi, (x - hi.astype(f32)).astype(bf16)


def layout(levels, tracers):
    group = 8 // math.gcd(levels, 8)
    chunks, q = [], 0
    while q < tracers:
        n = min(group, tracers - q)
        chunks.append((q * levels, -(-n * levels // 8) * 8, n * levels))
        q += n
    return chunks


def packing(levels, chunks):
    out = [(0, 1, 1)]
    for tiles in [c[1] // 8 for c in chunks] + [2 * (levels // 8) + 1] * 2:
        quads = (tiles - 1) // 4
        out.append((quads, tiles - quads, 8 * (tiles - quads)))
    return out


def kernel(
    sizes, dims,
    wind_h, temp_h, thick_h, tracer_h, ground_h, maps_h, det_h, ops_h, dct_h, wc_h,
    rot_h, flip_h, tally_h,
    wind_o, temp_o, thick_o, tracer_o, bound_o,
    wind, temp, thick, tracer, geo, ground, maps, det, ops, dct, wc,
    a_ref, b_ref, z_ref, below, above_ref, pack, seam_x, corner, total, peak,
    up_in, down_in, left_in, right_in, corner_in, total_in, peak_in,
    rot_ref, flip_ref, tally_ref,
    in_sem, sent_sem, piece_sem, side_sem, corner_sem, total_sem, peak_sem, chain_sem,
):
    nf, nt, nl = sizes
    levels, rows, columns, chunks, pad = dims
    derivative, weights = gll_tables()
    rep = [a - (a // 4) for a in range(rows)]
    distinct = rows - rows // 4 + 1
    face, tile, lev = lax.axis_index("face"), lax.axis_index("tile"), lax.axis_index("lev")
    f_up, f_dn = lax.rem(face + nf - 1, nf), lax.rem(face + 1, nf)
    t_lf, t_rt = lax.rem(tile + nt - 1, nt), lax.rem(tile + 1, nt)

    pieces = [(0, 8, 1)]
    at = 8
    for _, count, _ in chunks:
        pieces.append((at, count, 1))
        at += count
    pieces.append((at, 2 * pad, 1))
    pieces.append((at + 2 * pad, 2 * pad, 2))
    first_pack = np.cumsum([0] + [p[2] for p in pieces]).tolist()
    last = len(pieces) - 1
    heat = last - 1
    full, tail = levels // 8, levels % 8
    packed = packing(levels, chunks)
    first_row = np.cumsum([0] + [8 * p[1] for p in packed]).tolist()
    quarter = columns // 4
    side_rows = [1] + [8 * p[2] for p in pieces[1:]]

    n = levels * rows
    groups_in = [
        [(maps_h, maps), (det_h, det), (wc_h, wc),
         (wind_h.at[0], wind.at[0, :n]), (wind_h.at[1], wind.at[1, :n])],
        [(temp_h, temp.at[:n]), (thick_h, thick.at[:n])],
        [(ops_h, ops)],
        [(dct_h, dct), (ground_h, ground)],
    ]
    group_rows = [5 * rows + 1 + 2 * n, 2 * n, 5 * columns // 2, 3 * columns // 2 + rows]
    n0 = len(groups_in)
    spans = [pl.ds(start * rows, valid * rows) for start, _, valid in chunks]
    traced = [
        pltpu.make_async_copy(tracer_h.at[span], tracer.at[span], in_sem.at[n0 + k])
        for k, span in enumerate(spans)
    ]
    tables = [(rot_h, rot_ref), (flip_h, flip_ref), (tally_h, tally_ref)]
    at = n0 + len(chunks)
    tables = [pltpu.make_async_copy(s, d, in_sem.at[at + i]) for i, (s, d) in enumerate(tables)]

    def fetch(i):
        for s, d in groups_in[i]:
            pltpu.make_async_copy(s, d, in_sem.at[i]).start()

    def drain(count, sem):
        view = z_ref.at[0, pl.ds(0, count)] if count <= z_ref.shape[1] else tracer.at[pl.ds(0, count)]
        pltpu.make_async_copy(view, view, sem).wait()

    fetch(0)
    traced[0].start()
    fetch(2)
    fetch(1)
    for load in traced[1:]:
        load.start()
    fetch(3)
    for load in tables:
        load.start()

    diagonals = [(f_dn, t_rt, lev), (f_dn, t_lf, lev), (f_up, t_rt, lev), (f_up, t_lf, lev)]
    barrier = pltpu.get_barrier_semaphore()

    def notify(sem, to):
        pl.semaphore_signal(sem, inc=1, device_id=to, device_id_type=MESH)

    has_up, has_dn = face > 0, face < nf - 1
    at_end = face == nf - 1
    plane = [
        (face, lax.rem(tile + o, nt), lax.rem(lev + p, nl))
        for o in range(nt) for p in range(nl) if o or p
    ]

    def one(flag):
        return jnp.where(flag, 1, 0)

    for o in range(nf - 1, 1, -1):
        @pl.when(face + o < nf)
        def _():
            notify(barrier, (face + o, tile, lev))
    for here, other in ((has_up, face - 1), (has_dn, face + 1)):
        @pl.when(here)
        def _():
            for t in (tile, t_lf, t_rt):
                notify(barrier, (other, t, lev))

    @pl.when(face == 0)
    def _():
        for t in (t_lf, t_rt):
            notify(barrier, (nf - 1, t, lev))
    for o in range(nt):
        for p in range(nl):
            if o and p:
                @pl.when(tile + o < nt)
                def _():
                    notify(barrier, (face, tile + o, lax.rem(lev + p, nl)))
            elif o or p:
                notify(barrier, (face, lax.rem(tile + o, nt), lax.rem(lev + p, nl)))
    known = (
        nt - 1 + (nl - 1) * (1 + tile) + face + one(has_dn)
        + 2 * (one(has_up) + one(has_dn) + one(at_end))
    )
    unknown = (nt - 1 - tile) * (nl - 1) + jnp.maximum(nf - 2 - face, 0) + 2 * one(face == 0)

    def enter():
        pl.semaphore_wait(barrier, known)
        for o in range(2, nf):
            @pl.when(face - o >= 0)
            def _():
                notify(chain_sem.at[0], (face - o, tile, lev))

        @pl.when(at_end)
        def _():
            for t in (t_lf, t_rt):
                notify(chain_sem.at[0], (0, t, lev))
        for o in range(1, nt):
            for p in range(1, nl):
                @pl.when(tile - o >= 0)
                def _():
                    notify(chain_sem.at[0], (face, tile - o, lax.rem(lev + p, nl)))

    def ends_meet():
        @pl.when(unknown > 0)
        def _():
            pl.semaphore_wait(chain_sem.at[0], unknown)

    extra = (pad - levels) * rows
    if extra:
        zero = jnp.zeros((extra, columns), f32)
        temp[levels * rows :, :] = zero
        thick[levels * rows :, :] = zero
        geo[levels * rows :, :] = zero
        wind[0, levels * rows :, :] = zero
        wind[1, levels * rows :, :] = zero
    end = chunks[-1][0] + chunks[-1][2]
    more = chunks[-1][1] - chunks[-1][2]
    if more:
        tracer[end * rows :, :] = jnp.zeros((more * rows, columns), f32)

    sent = []

    def send(src, dst, r, to):
        pltpu.make_async_remote_copy(
            src_ref=src, dst_ref=dst, send_sem=sent_sem.at[0], recv_sem=r,
            device_id=to, device_id_type=MESH,
        ).start()
        sent.append(math.prod(src.shape) // columns)

    def column_sums():
        acc = jnp.zeros((rows, columns), f32)
        for k in reversed(range(levels)):
            term = temp[k * rows : (k + 1) * rows, :] * thick[k * rows : (k + 1) * rows, :]
            geo[k * rows : (k + 1) * rows, :] = acc + 0.5 * term
            acc = acc + term
        total[...] = acc

    def send_totals():
        for o in range(1, nl):
            send(total, total_in.at[o - 1], total_sem.at[0], (face, tile, lax.rem(lev + o, nl)))

    drain(group_rows[0], in_sem.at[0])
    w_col = wc[...]
    drain(group_rows[2], in_sem.at[2])
    table = ops[...]
    narrow = ops[: 2 * columns, :]
    wr = [float(weights[a % 4]) for a in range(rows)]
    m = [[maps[e * rows + a : e * rows + a + 1, :] for a in range(rows)] for e in range(4)]
    jac = [det[a : a + 1, :] for a in range(rows)]
    mass = [jac[a] * (wr[a] * w_col) for a in range(rows)]
    step_d = [[float(time_step * wr[a] * derivative[a % 4, b]) for b in range(4)] for a in range(rows)]
    dd = [[float(derivative[i, j]) for j in range(4)] for i in range(4)]

    def level_rows(ref, a):
        return ref[pl.ds(a, pad, stride=rows), :]

    def along_rows(values, a, coef):
        base = a - a % 4
        out = coef[0] * values[base]
        for b in range(1, 4):
            out = out + coef[b] * values[base + b]
        return out

    def merged(values):
        out = [None] * distinct
        for a in range(rows):
            r = rep[a]
            out[r] = values[a] if out[r] is None else out[r] + values[a]
        return out

    def lanes_plain(x):
        hi, lo = split(x)
        return jnp.dot(jnp.concatenate([hi, lo], 1), narrow, preferred_element_type=f32)

    def lanes_both(p, g):
        ph, plo = split(p)
        gh, glo = split(g)
        return jnp.dot(
            jnp.concatenate([ph, plo, gh, glo, gh], 1), table, preferred_element_type=f32
        )

    def by_column(values):
        stacked = jnp.concatenate(values, 0)
        hi, lo = split(stacked)
        out = jnp.dot(
            jnp.concatenate([hi, lo, hi], 1), dct[...], preferred_element_type=f32
        )
        n = values[0].shape[0]
        return [out[i * n : (i + 1) * n] for i in range(len(values))]

    lane = lax.broadcasted_iota(jnp.int32, (8, columns), 1)
    unit = 2 * distinct
    within = lax.rem(lane, unit)

    def put(piece, offset, r, z):
        z_ref[r, piece + offset : piece + offset + z.shape[0], :] = z

    def pack_of(start, groups):
        out = jnp.zeros((8, columns), f32)
        for i in range(groups):
            for r in range(distinct):
                spot = unit * i + 2 * r
                value = pltpu.roll(z_ref[r, start + 8 * i : start + 8 * i + 8, :], spot + 1, 1)
                out = jnp.where((lane == spot) | (lane == spot + 1), value, out)
        return out

    squeeze = jnp.minimum(lane + lane // 3, columns - 1)
    sublane = lax.broadcasted_iota(jnp.int32, (8, columns), 0)

    def tiles_of(j, r):
        start, count, _ = pieces[j]

        def tile_at(row):
            return z_ref[r, row : row + 8, :]

        if j < heat:
            return [tile_at(start + 8 * i) for i in range(count // 8)]
        out = [tile_at(start + half + 8 * i) for half in (0, pad) for i in range(full)]
        second = pltpu.roll(tile_at(start + pad + 8 * full), tail, 0)
        return out + [jnp.where(sublane < tail, tile_at(start + 8 * full), second)]

    def squeeze_rows(j):
        quads = packed[j][0]
        at = first_row[j]
        for r, out in ((distinct - 1, below), (0, above_ref)):
            wide = tiles_of(j, r)
            thin = [jnp.take_along_axis(x, squeeze, axis=1) for x in wide]
            done = []
            for g in range(quads):
                spare = thin[4 * g + 3]
                for t in range(3):
                    done.append(jnp.where(
                        lane < 3 * quarter, thin[4 * g + t],
                        pltpu.roll(spare, (3 - t) * quarter, 1),
                    ))
            done += thin[4 * quads :]
            for i in range(4 * quads):
                spot = 3 * quarter + 1 + i
                done[-1] = jnp.where(
                    lane == spot, pltpu.roll(wide[i], (spot + 1) % columns, 1), done[-1]
                )
            for i, x in enumerate(done):
                out[at + 8 * i : at + 8 * i + 8, :] = x

    def row_copy(j, down):
        height = packed[j][2]
        if j == 0:
            span = pl.ds(0, 1)
            source = z_ref.at[distinct - 1 if down else 0, span]
        else:
            span = pl.ds(first_row[j], height)
            source = (below if down else above_ref).at[span]
        landing = up_in if down else down_in
        send(source, landing.at[span], piece_sem.at[j], (f_dn if down else f_up, tile, lev))

    def ship_near(j):
        row_copy(j, True)

        @pl.when(has_up)
        def _():
            row_copy(j, False)
        sent.pop()

    def ship_wrap(j):
        @pl.when(face == 0)
        def _():
            row_copy(j, False)

    def ship_rows(j):
        row_copy(j, True)
        row_copy(j, False)

    def pack_sides(j):
        start, count, packs = pieces[j]
        each = count // packs
        made = []
        for p in range(packs):
            made.append(pack_of(start + p * each, each // 8))
            pack[first_pack[j] + p] = made[-1]
        return made

    def ship_sides(j):
        span = pl.ds(first_pack[j], pieces[j][2])
        for landing, to in ((left_in, (face, t_rt, lev)), (right_in, (face, t_lf, lev))):
            if j == 0:
                send(pack.at[0, pl.ds(0, 1)], landing.at[0, pl.ds(0, 1)], side_sem.at[0], to)
            else:
                send(pack.at[span], landing.at[span], side_sem.at[j], to)

    source = [unit - 2, unit - 1, 0, 1]

    def pack_corners(which, made):
        for d in range(4):
            out = jnp.zeros((8, columns), f32)
            for p, value in enumerate(made):
                out = jnp.where(within == p, pltpu.roll(value, (p - source[d]) % columns, 1), out)
            if which:
                folded = pltpu.roll(pltpu.roll(out, 4, 0), unit // 2, 1)
                out = jnp.where(within < unit // 2, out, folded)
            corner[which, d] = out

    def ship_corners(which):
        part = pl.ds(0, 4 if which else 1)
        for d in range(4):
            send(corner.at[which, d, part], corner_in.at[which, d, part],
                 corner_sem.at[which], diagonals[d])

    east = [level_rows(wind.at[0], a) for a in range(rows)]
    north = [level_rows(wind.at[1], a) for a in range(rows)]
    speed, parts = None, []
    whole = max(c[1] for c in chunks)
    for a in range(rows):
        aa = jac[a] * (m[0][a] * east[a] + m[1][a] * north[a])
        bb = jac[a] * (m[2][a] * east[a] + m[3][a] * north[a])
        parts.append(((aa * w_col)[:levels], (bb * wr[a])[:levels]))
        spacing = jnp.sqrt(
            m[0][a] * m[0][a] + m[1][a] * m[1][a] + m[2][a] * m[2][a] + m[3][a] * m[3][a]
        )
        here = jnp.max(east[a] * east[a] + north[a] * north[a], axis=0, keepdims=True)
        here = jnp.sqrt(here) * spacing
        speed = here if speed is None else jnp.maximum(speed, here)

    @pl.when(face < nf)
    def _():
        for a, pair in enumerate(parts):
            for k in range(-(-whole // levels)):
                n = min(levels, whole - k * levels)
                a_ref[a, k * levels : k * levels + n, :] = pair[0][:n]
                b_ref[a, k * levels : k * levels + n, :] = pair[1][:n]

    def put_mass():
        whole_rows = lanes_plain(jnp.concatenate(
            [jnp.broadcast_to(x, (8, columns)) for x in merged(mass)], 0
        ))
        for r in range(distinct):
            put(0, 0, r, whole_rows[8 * r : 8 * r + 8])

    def tracers_of(k):
        start, count, _ = chunks[k]
        q = [tracer[pl.ds(start * rows + a, count, stride=rows), :] for a in range(rows)]
        first = [q[a] * a_ref[a, :count, :] for a in range(rows)]
        keep = [mass[a] * q[a] - along_rows(first, a, step_d[a]) for a in range(rows)]
        second = [q[a] * b_ref[a, :count, :] for a in range(rows)]
        for r, (x, y) in enumerate(zip(merged(keep), merged(second))):
            put(pieces[k + 1][0], 0, r, lanes_both(x, y))


    def ready(j):
        squeeze_rows(j)
        return pack_sides(j)

    traced[0].wait()
    tracers_of(0)
    made = ready(1)
    enter()
    ship_near(1)
    ship_sides(1)

    drain(group_rows[1], in_sem.at[1])
    traced[1].wait()
    column_sums()
    put_mass()
    tracers_of(1)
    mass_made = pack_sides(0)
    pack_corners(0, mass_made)
    made += ready(2)
    send_totals()
    ship_near(2)
    ship_sides(2)
    ship_near(0)
    ship_sides(0)

    drain(group_rows[3], in_sem.at[3])
    traced[2].wait()
    tracers_of(2)
    depth = [level_rows(thick, a) for a in range(rows)]
    depth_c = by_column(depth)
    flux_a, flux_b = [], []
    for a in range(rows):
        dr, dc = along_rows(depth, a, dd[a % 4]), depth_c[a]
        gx, gy = m[0][a] * dr + m[2][a] * dc, m[1][a] * dr + m[3][a] * dc
        flux_a.append(jac[a] * (m[0][a] * gx + m[1][a] * gy))
        flux_b.append(jac[a] * (m[2][a] * gx + m[3][a] * gy))
    flux_c = by_column(flux_b)
    damp = None
    for a in range(rows):
        lap = jnp.abs(along_rows(flux_a, a, dd[a % 4]) + flux_c[a])
        here = jnp.max(lap, axis=0, keepdims=True) / jac[a]
        damp = here if damp is None else jnp.maximum(damp, here)
    peak[0] = jnp.concatenate(
        [time_step * speed, (time_step * viscosity) * damp, jnp.zeros((6, columns), f32)], 0
    )
    first, second, keep = [], [], []
    for a in range(rows):
        aa = jac[a] * (m[0][a] * east[a] + m[1][a] * north[a])
        bb = jac[a] * (m[2][a] * east[a] + m[3][a] * north[a])
        first.append(w_col * (depth[a] * aa - viscosity * flux_a[a]))
        second.append(wr[a] * (depth[a] * bb - viscosity * flux_b[a]))
    for a in range(rows):
        keep.append(mass[a] * depth[a] - along_rows(first, a, step_d[a]))
    for r, (x, y) in enumerate(zip(merged(keep), merged(second))):
        put(pieces[heat][0], pad, r, lanes_both(x, y))
    warm = [level_rows(temp, a) for a in range(rows)]
    warm_c = by_column(warm)
    value = []
    for a in range(rows):
        dr, dc = along_rows(warm, a, dd[a % 4]), warm_c[a]
        gx, gy = m[0][a] * dr + m[2][a] * dc, m[1][a] * dr + m[3][a] * dc
        value.append(mass[a] * (warm[a] - time_step * (east[a] * gx + north[a] * gy)))
    for r, x in enumerate(merged(value)):
        put(pieces[heat][0], 0, r, lanes_plain(x))
    made += ready(3)
    made += ready(heat)
    ship_near(3)
    ship_sides(3)
    ship_near(heat)
    ship_sides(heat)

    traced[3].wait()
    tracers_of(3)
    pack_corners(1, made)
    later = ready(4)
    ends_meet()
    ship_corners(0)
    for o, peer in enumerate(plane):
        send(peak.at[0, pl.ds(0, 2)], peak_in.at[o, pl.ds(0, 2)], peak_sem.at[0], peer)
    ship_near(4)
    ship_sides(4)
    ship_corners(1)
    for j in (0, 1, 2, 3, heat, 4):
        ship_wrap(j)

    if nl > 1:
        drain((nl - 1) * rows, total_sem.at[0])
    traced[4].wait()
    above = ground[...]
    for o in range(nl - 1):
        origin = lax.rem(lev + nl - (o + 1), nl)
        use = jnp.where(origin > lev, 1.0, 0.0).astype(f32)
        above = above + use * total_in[o]
    energy = []
    for a in range(rows):
        u, v = level_rows(wind.at[0], a), level_rows(wind.at[1], a)
        energy.append(0.5 * (u * u + v * v) + level_rows(geo, a) + above[a : a + 1, :])
    energy_c = by_column(energy)
    value_u, value_v = [], []
    for a in range(rows):
        u, v = level_rows(wind.at[0], a), level_rows(wind.at[1], a)
        dr, dc = along_rows(energy, a, dd[a % 4]), energy_c[a]
        value_u.append(mass[a] * (u - time_step * (m[0][a] * dr + m[2][a] * dc)))
        value_v.append(mass[a] * (v - time_step * (m[1][a] * dr + m[3][a] * dc)))
    for r, (x, y) in enumerate(zip(merged(value_u), merged(value_v))):
        put(pieces[last][0], 0, r, lanes_plain(x))
        put(pieces[last][0], pad, r, lanes_plain(y))
    tracers_of(4)
    later += ready(last)
    later += ready(5)
    pack_corners(2, later)
    ship_sides(last)
    ship_sides(5)
    ship_corners(2)
    ship_rows(last)
    ship_rows(5)

    def spread_peaks():
        best = peak[0]
        if plane:
            drain(2 * len(plane), peak_sem.at[0])
        for o in range(len(plane)):
            best = jnp.maximum(best, peak_in[o])
        peak[1] = best
        for o in range(1, nf):
            send(peak.at[1, pl.ds(0, 2)], peak_in.at[len(plane) + o - 1, pl.ds(0, 2)],
                 peak_sem.at[1], (lax.rem(face + o, nf), tile, lev))

    spread_peaks()

    def gathered(stage, base, count):
        best = peak[stage]
        if count:
            drain(2 * count, peak_sem.at[stage])
        for o in range(count):
            best = jnp.maximum(best, peak_in[base + o])
        return best

    for load in tables:
        load.wait()

    def seam(ref, f, t, k):
        return ref[f, k, t]

    codes = [
        lax.rem(4 - seam(rot_ref, f_up, tile, 0), 4), seam(rot_ref, face, tile, 0),
        lax.rem(4 - seam(rot_ref, face, t_lf, 1), 4), seam(rot_ref, face, tile, 1),
    ]
    flips = [
        seam(flip_ref, f_up, tile, 0), seam(flip_ref, face, tile, 0),
        seam(flip_ref, face, t_lf, 1), seam(flip_ref, face, tile, 1),
    ]
    tallies = [
        tally_ref[f_up, t_lf], tally_ref[f_up, tile],
        tally_ref[face, t_lf], tally_ref[face, tile],
    ]

    def cosine(code):
        return jnp.where(code == 0, 1.0, jnp.where(code == 2, -1.0, 0.0)).astype(f32)

    def sine(code):
        return jnp.where(code == 1, 1.0, jnp.where(code == 3, -1.0, 0.0)).astype(f32)

    def filled(x):
        return jnp.full((8, columns), x)

    odd = lax.rem(lane, 2) == 1
    mirror = lane - within + (unit - 2) - 2 * (within // 2) + lax.rem(within, 2)
    mirror = jnp.clip(mirror, 0, columns - 1)
    side_flip = jnp.where(odd, filled(flips[2]), filled(flips[3])) == 1
    side_cos = jnp.where(odd, filled(cosine(codes[2])), filled(cosine(codes[3])))
    side_sin = jnp.where(odd, filled(sine(codes[2])), filled(sine(codes[3])))
    corner_code = [
        lax.rem(codes[0] + codes[2], 4), lax.rem(codes[0] + codes[3], 4),
        lax.rem(codes[1] + codes[2], 4), lax.rem(codes[1] + codes[3], 4),
    ]
    target = [1, 0, unit - 1, unit - 2]
    alive = [filled(tallies[d]) == 4 for d in range(4)]

    def sides(index):
        if index == 0:
            a = jnp.broadcast_to(left_in[0, 0:1, :], (8, columns))
            b = jnp.broadcast_to(right_in[0, 0:1, :], (8, columns))
        else:
            a, b = left_in[index], right_in[index]
        x = jnp.where(odd, pltpu.roll(a, 1, 1), pltpu.roll(b, columns - 1, 1))
        return jnp.where(side_flip, jnp.take_along_axis(x, mirror, axis=1), x)

    def corner_tile(which, d):
        if which == 0:
            return jnp.broadcast_to(corner_in[0, d, 0:1, :], (8, columns))
        x = corner_in[which, d]
        lower = pltpu.roll(pltpu.roll(x, 4, 0), columns - unit // 2, 1)
        return jnp.where(sublane < 4, x, lower)

    def corner_values(which, d, p):
        x = corner_tile(which, d)
        x = pltpu.roll(x, (target[d] - p) % columns, 1)
        return jnp.where(alive[d] & (within == target[d]), x, 0.0)

    edge = (lane[:1] == 0) | (lane[:1] == columns - 1)

    def to_edges(x, i, r):
        y = pltpu.roll(x, (columns - (unit * i + 2 * r + 1)) % columns, 1)
        return jnp.where(edge, y, 0.0)

    rev = (columns - 1) - lane
    row_flip = [filled(flips[0]) == 1, filled(flips[1]) == 1]
    origin_lane = [jnp.where(row_flip[i], rev, lane) for i in range(2)]
    spread = [x - x // 4 for x in origin_lane]
    inner = [jnp.minimum(x, 3 * quarter - 1) for x in spread]
    rim_end = [x == columns - 1 for x in origin_lane]

    def row_rim(ref, which, j):
        if j == 0:
            x = jnp.broadcast_to(ref[0:1, :], (8, columns))
            return [jnp.take_along_axis(x, origin_lane[which], axis=1)]
        quads, width, _ = packed[j]
        at = first_row[j]
        got = [ref[at + 8 * i : at + 8 * i + 8, :] for i in range(width)]
        ends = got[-1]
        out = []
        for g in range(quads):
            one, two, three = got[3 * g : 3 * g + 3]
            four = jnp.where(
                lane < quarter, pltpu.roll(one, quarter, 1),
                jnp.where(lane < 2 * quarter, pltpu.roll(two, 2 * quarter, 1),
                          pltpu.roll(three, 3 * quarter, 1)),
            )
            for x in (one, two, three, four):
                spot = 3 * quarter + 1 + len(out)
                x = jnp.take_along_axis(x, inner[which], axis=1)
                end = jnp.broadcast_to(ends[:, spot : spot + 1], (8, columns))
                out.append(jnp.where(rim_end[which], end, x))
        for x in got[3 * quads :]:
            out.append(jnp.take_along_axis(x, spread[which], axis=1))
        if j >= heat:
            second = pltpu.roll(out[-1], 8 - tail, 0)
            out = out[:full] + out[-1:] + out[full : 2 * full] + [second]
        return out

    sets = [[0], [1, 2, 3, heat], [4, last, last, 5]]
    corner_spot = {j: (w, group.index(j)) for w, group in enumerate(sets) for j in group}

    def sides_of(j):
        p = first_pack[j]
        if j < last:
            return [sides(p)]
        xu, xv = sides(p), sides(p + 1)
        return [side_cos * xu - side_sin * xv, side_sin * xu + side_cos * xv]

    def with_corners(j):
        which, p = corner_spot[j]
        if j < last:
            return [seam_x[first_pack[j]] + sum_corners(which, p)]
        xu, xv = seam_x[first_pack[j]], seam_x[first_pack[j] + 1]
        for d in range(4):
            cu, cv = corner_values(which, d, p), corner_values(which, d, p + 1)
            c, s = cosine(corner_code[d]), sine(corner_code[d])
            xu, xv = xu + (c * cu - s * cv), xv + (s * cu + c * cv)
        return [xu, xv]

    def sum_corners(which, p):
        parts = [corner_values(which, d, p) for d in range(4)]
        return parts[0] + parts[1] + parts[2] + parts[3]

    def rims_of(j):
        both = [row_rim(up_in, 0, j), row_rim(down_in, 1, j)]
        if j == last:
            for which in range(2):
                x = both[which]
                c, s = cosine(codes[which]), sine(codes[which])
                ru = [c * x[i] - s * x[groups + i] for i in range(groups)]
                rv = [s * x[i] + c * x[groups + i] for i in range(groups)]
                both[which] = ru + rv
        return both

    def stored(ref, begin, i, valid, r, x):
        n = min(8, valid - 8 * i)
        for a in range(rows):
            if rep[a] == r:
                ref[pl.ds((begin + 8 * i) * rows + a, n, stride=rows), :] = (x * inverse[a])[:n]

    inverse = [None] * rows
    insides, borders = range(1, distinct - 1), (0, distinct - 1)

    def finish(j, seams, which_rows, both=None):
        start, total_count, packs = pieces[j]
        each = (total_count // packs) // 8
        for i in range(total_count // 8):
            for r in which_rows:
                x = z_ref[r, start + 8 * i : start + 8 * i + 8, :]
                x = x + to_edges(seams[i // each], i % each, r)
                if r in borders:
                    x = x + both[0 if r == 0 else 1][i]
                if j == 0:
                    for a in range(rows):
                        if rep[a] == r:
                            inverse[a] = 1.0 / x
                elif j < heat:
                    begin, _, valid = chunks[j - 1]
                    stored(tracer_o, begin, i, valid, r, x)
                else:
                    first_half, k = i < groups, i % groups
                    if j == heat:
                        ref = temp_o if first_half else thick_o
                    else:
                        ref = wind_o.at[0 if first_half else 1]
                    stored(ref, 0, k, levels, r, x)

    groups = pad // 8
    order = [0, 1, 2, 3, heat, 4, last, 5]
    for j in order:
        drain(2 * side_rows[j], side_sem.at[j])
    for j in order:
        seams = sides_of(j)
        for i, x in enumerate(seams):
            seam_x[first_pack[j] + i] = x
        finish(j, seams, insides)
    for block in (sets[0] + sets[1], list(dict.fromkeys(sets[2]))):
        for j in block:
            drain(2 * packed[j][2], piece_sem.at[j])
        if 0 in block:
            drain(4, corner_sem.at[0])
        drain(16, corner_sem.at[1 if 0 in block else 2])
        for j in block:
            finish(j, with_corners(j), borders, rims_of(j))

    bound_o[...] = gathered(1, len(plane), nf - 1)
    drain(sum(sent), sent_sem.at[0])


def write_out(wind, temp, thick, tracer, bound, wind_o, temp_o, thick_o, tracer_o, bound_o, sem):
    pairs = ((tracer, tracer_o), (wind, wind_o), (temp, temp_o), (thick, thick_o))
    copies = [pltpu.make_async_copy(a, b, sem.at[i]) for i, (a, b) in enumerate(pairs)]
    for copy in copies:
        copy.start()
    bound_o[0] = jnp.max(bound[0:1, :])
    bound_o[1] = jnp.max(bound[1:2, :])
    for copy in copies:
        copy.wait()


def on_device(
    sizes, wind, temp, thick, tracers, ground, maps, det, rot, flip, tally
):
    nf, nt, nl = sizes
    levels, rows, columns = temp.shape
    count = tracers.shape[0]
    chunks = layout(levels, count)
    pad = -(-levels // 8) * 8
    if rows != 8 or columns != 128 or levels % 8 not in (1, 2, 3, 4) or len(chunks) != 5:
        raise ValueError("block shape")
    table, dct, w_col = lane_tables(columns)
    distinct = rows - rows // 4 + 1
    total_rows = 4 * pad + 8 + sum(c[1] for c in chunks)
    pieces = len(chunks) + 3
    packs = len(chunks) + 4
    landing = sum(8 * p[1] for p in packing(levels, chunks))
    whole = max(c[1] for c in chunks)
    n = levels * rows
    dma = pltpu.SemaphoreType.DMA
    peers = nt * nl - 1 + nf - 1
    hbm = pl.BlockSpec(memory_space=pl.ANY)
    smem = pl.BlockSpec(memory_space=pltpu.SMEM)
    vmem = pl.BlockSpec(memory_space=pltpu.VMEM)
    last = chunks[-1]
    shapes = ((2, n, columns), (n, columns), (n, columns), (count * n, columns), (8, columns))
    outs = pl.pallas_call(
        functools.partial(kernel, sizes, (levels, rows, columns, chunks, pad)),
        out_shape=tuple(pltpu.VMEM(shape, f32) for shape in shapes),
        in_specs=[hbm] * 13,
        out_specs=(vmem,) * 5,
        scratch_shapes=[
            pltpu.VMEM((2, pad * rows, columns), f32),
            pltpu.VMEM((pad * rows, columns), f32),
            pltpu.VMEM((pad * rows, columns), f32),
            pltpu.VMEM(((last[0] + last[1]) * rows, columns), f32),
            pltpu.VMEM((pad * rows, columns), f32),
            pltpu.VMEM((rows, columns), f32),
            pltpu.VMEM((4 * rows, columns), f32),
            pltpu.VMEM((rows, columns), f32),
            pltpu.VMEM(table.shape, bf16),
            pltpu.VMEM(dct.shape, bf16),
            pltpu.VMEM((1, columns), f32),
            pltpu.VMEM((rows, whole, columns), f32),
            pltpu.VMEM((rows, whole, columns), f32),
            pltpu.VMEM((distinct, total_rows, columns), f32),
            pltpu.VMEM((landing, columns), f32),
            pltpu.VMEM((landing, columns), f32),
            pltpu.VMEM((packs, 8, columns), f32),
            pltpu.VMEM((packs, 8, columns), f32),
            pltpu.VMEM((3, 4, 8, columns), f32),
            pltpu.VMEM((rows, columns), f32),
            pltpu.VMEM((2, 8, columns), f32),
            pltpu.VMEM((landing, columns), f32),
            pltpu.VMEM((landing, columns), f32),
            pltpu.VMEM((packs, 8, columns), f32),
            pltpu.VMEM((packs, 8, columns), f32),
            pltpu.VMEM((3, 4, 8, columns), f32),
            pltpu.VMEM((nl - 1, rows, columns), f32),
            pltpu.VMEM((peers, 8, columns), f32),
            pltpu.SMEM((nf, 2, nt), jnp.int32),
            pltpu.SMEM((nf, 2, nt), jnp.int32),
            pltpu.SMEM((nf, nt), jnp.int32),
            dma((7 + len(chunks),)),
            dma((1,)),
            dma((pieces,)),
            dma((pieces,)),
            dma((3,)),
            dma((1,)),
            dma((2,)),
            pltpu.SemaphoreType.REGULAR((1,)),
        ],
        compiler_params=pltpu.CompilerParams(collective_id=0, has_side_effects=True),
    )(
        wind.reshape(2, n, columns), temp.reshape(n, columns), thick.reshape(n, columns),
        tracers.reshape(count * n, columns), ground, maps.reshape(4 * rows, columns), det,
        table, dct, w_col, rot.transpose(0, 2, 1), flip.transpose(0, 2, 1), tally,
    )
    outs = pl.pallas_call(
        write_out,
        out_shape=tuple(jax.ShapeDtypeStruct(x, f32) for x in shapes[:4] + ((2,),)),
        in_specs=[vmem] * 5,
        out_specs=(hbm,) * 4 + (smem,),
        scratch_shapes=[dma((4,))],
    )(*[pltpu.with_memory_space_constraint(x, pltpu.VMEM) for x in outs])
    return (
        outs[0].reshape(wind.shape), outs[1].reshape(temp.shape), outs[2].reshape(thick.shape),
        outs[3].reshape(tracers.shape), outs[4],
    )


def solution(mesh):
    sizes = tuple(mesh.shape[name] for name in ("face", "tile", "lev"))
    level = P("lev", "face", "tile")
    stacked = P(None, "lev", "face", "tile")
    return jax.shard_map(
        functools.partial(on_device, sizes),
        mesh=mesh,
        in_specs=(stacked, level, level, stacked, P("face", "tile"), P(None, "face", "tile"),
                  P("face", "tile"), P(), P(), P()),
        out_specs=(stacked, level, level, stacked, P()),
        check_vma=False,
    )
```

```python
import functools
import math

import jax
import jax.numpy as jnp
import numpy as np
from jax import lax
from jax.experimental import pallas as pl
from jax.experimental.pallas import tpu as pltpu
from jax.sharding import PartitionSpec as P

time_step = 0.05
viscosity = 0.05
f32 = jnp.float32
bf16 = jnp.bfloat16
MESH = pl.DeviceIdType.MESH
highest = lax.Precision.HIGHEST


def gll_tables():
    offset = 1.0 / math.sqrt(5.0)
    nodes = np.array([-1.0, -offset, offset, 1.0])
    weights = np.array([1.0 / 6.0, 5.0 / 6.0, 5.0 / 6.0, 1.0 / 6.0])
    bary = np.ones(4)
    for i in range(4):
        for j in range(4):
            if j != i:
                bary[i] = bary[i] / (nodes[i] - nodes[j])
    derivative = np.zeros((4, 4))
    for i in range(4):
        for j in range(4):
            if j != i:
                derivative[i, j] = bary[j] / bary[i] / (nodes[i] - nodes[j])
        derivative[i, i] = -np.sum(derivative[i])
    return derivative, weights


def lane_tables(columns):
    derivative, weights = gll_tables()
    d = np.kron(np.eye(columns // 4), derivative)
    s = np.eye(columns)
    for c in range(columns - 1):
        if c % 4 == 3:
            s[c, c + 1] = s[c + 1, c] = 1.0
    w = np.tile(weights, columns // 4)
    t = (-time_step * (d.T * w[None, :]) @ s).astype(np.float32)
    t_hi = jnp.asarray(t).astype(bf16)
    t_lo = (jnp.asarray(t) - t_hi.astype(f32)).astype(bf16)
    sb = jnp.asarray(s, bf16)
    d_t = jnp.asarray(d.T, f32)
    d_hi = d_t.astype(bf16)
    d_lo = (d_t - d_hi.astype(f32)).astype(bf16)
    return jnp.concatenate([sb, sb, t_hi, t_hi, t_lo], 0), jnp.concatenate([d_hi, d_hi, d_lo], 0), jnp.asarray(w[None, :], f32)


def split(x):
    hi = x.astype(bf16)
    return hi, (x - hi.astype(f32)).astype(bf16)


def layout(levels, tracers):
    group = 8 // math.gcd(levels, 8)
    chunks, q = [], 0
    while q < tracers:
        n = min(group, tracers - q)
        chunks.append((q * levels, -(-n * levels // 8) * 8, n * levels))
        q += n
    return chunks


def packing(levels, chunks):
    sizes = [(c[1] // 8, c[2] - (c[1] - 8)) for c in chunks]
    sizes += [(2 * (levels // 8) + 1, 2 * (levels % 8))] * 2
    out = [(0, 1, 1)]
    for tiles, left in sizes:
        quads = (tiles - 1) // 4
        width = tiles - quads
        out.append((quads, width, 8 * width - (4 if left <= 4 else 0)))
    return out


def kernel(
    sizes, dims,
    wind_h, temp_h, thick_h, tracer_h, ground_h, maps_h, det_h, ops_h, dct_h, wc_h,
    rot_h, flip_h, tally_h,
    wind_o, temp_o, thick_o, tracer_o, bound_o,
    wind, temp, thick, tracer, geo, ground, maps, det, ops, dct, wc,
    a_ref, b_ref, z_ref, below, above_ref, pack, seam_x, corner, total, peak,
    up_in, down_in, left_in, right_in, corner_in, total_in, peak_in,
    rot_ref, flip_ref, tally_ref,
    in_sem, sent_sem, piece_sem, side_sem, corner_sem, total_sem, peak_sem, chain_sem,
):
    nf, nt, nl = sizes
    levels, rows, columns, chunks, pad = dims
    derivative, weights = gll_tables()
    rep = [a - (a // 4) for a in range(rows)]
    distinct = rows - rows // 4 + 1
    face, tile, lev = lax.axis_index("face"), lax.axis_index("tile"), lax.axis_index("lev")
    f_up, f_dn = lax.rem(face + nf - 1, nf), lax.rem(face + 1, nf)
    t_lf, t_rt = lax.rem(tile + nt - 1, nt), lax.rem(tile + 1, nt)

    pieces = [(0, 8, 1)]
    at = 8
    for _, count, _ in chunks:
        pieces.append((at, count, 1))
        at += count
    pieces.append((at, 2 * pad, 1))
    pieces.append((at + 2 * pad, 2 * pad, 2))
    first_pack = np.cumsum([0] + [p[2] for p in pieces]).tolist()
    last = len(pieces) - 1
    heat = last - 1
    full, tail = levels // 8, levels % 8
    packed = packing(levels, chunks)
    first_row = np.cumsum([0] + [8 * p[1] for p in packed]).tolist()
    quarter = columns // 4
    side_rows = [1] + [8 * p[2] for p in pieces[1:]]

    n = levels * rows
    groups_in = [
        [(maps_h, maps), (det_h, det), (wc_h, wc),
         (wind_h.at[0], wind.at[0, :n]), (wind_h.at[1], wind.at[1, :n])],
        [(temp_h, temp.at[:n]), (thick_h, thick.at[:n])],
        [(ops_h, ops)],
        [(dct_h, dct), (ground_h, ground)],
    ]
    group_rows = [5 * rows + 1 + 2 * n, 2 * n, 5 * columns // 2, 3 * columns // 2 + rows]
    n0 = len(groups_in)
    spans = [pl.ds(start * rows, valid * rows) for start, _, valid in chunks]
    traced = [
        pltpu.make_async_copy(tracer_h.at[span], tracer.at[span], in_sem.at[n0 + k])
        for k, span in enumerate(spans)
    ]
    tables = [(rot_h, rot_ref), (flip_h, flip_ref), (tally_h, tally_ref)]
    at = n0 + len(chunks)
    tables = [pltpu.make_async_copy(s, d, in_sem.at[at + i]) for i, (s, d) in enumerate(tables)]

    def fetch(i):
        for s, d in groups_in[i]:
            pltpu.make_async_copy(s, d, in_sem.at[i]).start()

    def drain(count, sem):
        view = z_ref.at[0, pl.ds(0, count)] if count <= z_ref.shape[1] else tracer.at[pl.ds(0, count)]
        pltpu.make_async_copy(view, view, sem).wait()

    fetch(0)
    traced[0].start()
    fetch(2)
    fetch(1)
    for load in traced[1:]:
        load.start()
    fetch(3)
    for load in tables:
        load.start()

    diagonals = [(f_dn, t_rt, lev), (f_dn, t_lf, lev), (f_up, t_rt, lev), (f_up, t_lf, lev)]
    barrier = pltpu.get_barrier_semaphore()

    def notify(sem, to):
        pl.semaphore_signal(sem, inc=1, device_id=to, device_id_type=MESH)

    has_up, has_dn = face > 0, face < nf - 1
    at_end = face == nf - 1
    plane = [
        (face, lax.rem(tile + o, nt), lax.rem(lev + p, nl))
        for o in range(nt) for p in range(nl) if o or p
    ]

    def one(flag):
        return jnp.where(flag, 1, 0)

    for o in range(nf - 1, 1, -1):
        @pl.when(face + o < nf)
        def _():
            notify(barrier, (face + o, tile, lev))
    for here, other in ((has_up, face - 1), (has_dn, face + 1)):
        @pl.when(here)
        def _():
            for t in (tile, t_lf, t_rt):
                notify(barrier, (other, t, lev))

    @pl.when(face == 0)
    def _():
        for t in (t_lf, t_rt):
            notify(barrier, (nf - 1, t, lev))
    for o in range(nt):
        for p in range(nl):
            if o and p:
                @pl.when(tile + o < nt)
                def _():
                    notify(barrier, (face, tile + o, lax.rem(lev + p, nl)))
            elif o or p:
                notify(barrier, (face, lax.rem(tile + o, nt), lax.rem(lev + p, nl)))
    known = (
        nt - 1 + (nl - 1) * (1 + tile) + face + one(has_dn)
        + 2 * (one(has_up) + one(has_dn) + one(at_end))
    )
    unknown = jnp.maximum(nf - 2 - face, 0) + 2 * one(face == 0)
    beside = (nt - 1 - tile) * (nl - 1)

    def enter():
        pl.semaphore_wait(barrier, known)
        for o in range(2, nf):
            @pl.when(face - o >= 0)
            def _():
                notify(chain_sem.at[0], (face - o, tile, lev))

        @pl.when(at_end)
        def _():
            for t in (t_lf, t_rt):
                notify(chain_sem.at[0], (0, t, lev))
        for o in range(1, nt):
            for p in range(1, nl):
                @pl.when(tile - o >= 0)
                def _():
                    notify(chain_sem.at[1], (face, tile - o, lax.rem(lev + p, nl)))

    def plane_meets():
        @pl.when(beside > 0)
        def _():
            pl.semaphore_wait(chain_sem.at[1], beside)

    def ends_meet():
        @pl.when(unknown > 0)
        def _():
            pl.semaphore_wait(chain_sem.at[0], unknown)

    extra = (pad - levels) * rows
    if extra:
        zero = jnp.zeros((extra, columns), f32)
        temp[levels * rows :, :] = zero
        thick[levels * rows :, :] = zero
        geo[levels * rows :, :] = zero
        wind[0, levels * rows :, :] = zero
        wind[1, levels * rows :, :] = zero
    end = chunks[-1][0] + chunks[-1][2]
    more = chunks[-1][1] - chunks[-1][2]
    if more:
        tracer[end * rows :, :] = jnp.zeros((more * rows, columns), f32)

    sent = []

    def send(src, dst, r, to):
        pltpu.make_async_remote_copy(
            src_ref=src, dst_ref=dst, send_sem=sent_sem.at[0], recv_sem=r,
            device_id=to, device_id_type=MESH,
        ).start()
        sent.append(math.prod(src.shape) // columns)

    def column_sums():
        acc = jnp.zeros((rows, columns), f32)
        for k in reversed(range(levels)):
            term = temp[k * rows : (k + 1) * rows, :] * thick[k * rows : (k + 1) * rows, :]
            geo[k * rows : (k + 1) * rows, :] = acc + 0.5 * term
            acc = acc + term
        total[...] = acc

    def send_totals():
        for o in range(1, nl):
            send(total, total_in.at[o - 1], total_sem.at[0], (face, tile, lax.rem(lev + o, nl)))

    drain(group_rows[0], in_sem.at[0])
    w_col = wc[...]
    drain(group_rows[2], in_sem.at[2])
    table = ops[...]
    narrow = ops[: 2 * columns, :]
    wr = [float(weights[a % 4]) for a in range(rows)]
    m = [[maps[e * rows + a : e * rows + a + 1, :] for a in range(rows)] for e in range(4)]
    jac = [det[a : a + 1, :] for a in range(rows)]
    mass = [jac[a] * (wr[a] * w_col) for a in range(rows)]
    step_d = [[float(time_step * wr[a] * derivative[a % 4, b]) for b in range(4)] for a in range(rows)]
    dd = [[float(derivative[i, j]) for j in range(4)] for i in range(4)]

    def level_rows(ref, a):
        return ref[pl.ds(a, pad, stride=rows), :]

    def along_rows(values, a, coef):
        base = a - a % 4
        out = coef[0] * values[base]
        for b in range(1, 4):
            out = out + coef[b] * values[base + b]
        return out

    def merged(values):
        out = [None] * distinct
        for a in range(rows):
            r = rep[a]
            out[r] = values[a] if out[r] is None else out[r] + values[a]
        return out

    def lanes_plain(x):
        hi, lo = split(x)
        return jnp.dot(jnp.concatenate([hi, lo], 1), narrow, preferred_element_type=f32)

    def lanes_both(p, g):
        ph, plo = split(p)
        gh, glo = split(g)
        return jnp.dot(
            jnp.concatenate([ph, plo, gh, glo, gh], 1), table, preferred_element_type=f32
        )

    def by_column(values):
        stacked = jnp.concatenate(values, 0)
        hi, lo = split(stacked)
        out = jnp.dot(
            jnp.concatenate([hi, lo, hi], 1), dct[...], preferred_element_type=f32
        )
        n = values[0].shape[0]
        return [out[i * n : (i + 1) * n] for i in range(len(values))]

    lane = lax.broadcasted_iota(jnp.int32, (8, columns), 1)
    unit = 2 * distinct
    within = lax.rem(lane, unit)

    def put(piece, offset, r, z):
        z_ref[r, piece + offset : piece + offset + z.shape[0], :] = z

    def pack_of(start, groups):
        out = jnp.zeros((8, columns), f32)
        for i in range(groups):
            for r in range(distinct):
                spot = unit * i + 2 * r
                value = pltpu.roll(z_ref[r, start + 8 * i : start + 8 * i + 8, :], spot + 1, 1)
                out = jnp.where((lane == spot) | (lane == spot + 1), value, out)
        return out

    squeeze = jnp.minimum(lane + lane // 3, columns - 1)
    sublane = lax.broadcasted_iota(jnp.int32, (8, columns), 0)

    def tiles_of(j, r):
        start, count, _ = pieces[j]

        def tile_at(row):
            return z_ref[r, row : row + 8, :]

        if j < heat:
            return [tile_at(start + 8 * i) for i in range(count // 8)]
        out = [tile_at(start + half + 8 * i) for half in (0, pad) for i in range(full)]
        second = pltpu.roll(tile_at(start + pad + 8 * full), tail, 0)
        return out + [jnp.where(sublane < tail, tile_at(start + 8 * full), second)]

    def end_spots(j, i, x):
        spot = 3 * quarter + 1
        if packed[j][2] % 8 == 0:
            return [(spot + i, x)]
        return [(spot + 2 * i, x), (spot + 2 * i + 1, pltpu.roll(x, 4, 0))]

    def squeeze_rows(j):
        quads = packed[j][0]
        at = first_row[j]
        for r, out in ((distinct - 1, below), (0, above_ref)):
            wide = tiles_of(j, r)
            thin = [jnp.take_along_axis(x, squeeze, axis=1) for x in wide]
            done = []
            for g in range(quads):
                spare = thin[4 * g + 3]
                for t in range(3):
                    done.append(jnp.where(
                        lane < 3 * quarter, thin[4 * g + t],
                        pltpu.roll(spare, (3 - t) * quarter, 1),
                    ))
            done += thin[4 * quads :]
            for i in range(4 * quads):
                for spot, x in end_spots(j, i, wide[i]):
                    done[-1] = jnp.where(
                        lane == spot, pltpu.roll(x, (spot + 1) % columns, 1), done[-1]
                    )
            for i, x in enumerate(done):
                out[at + 8 * i : at + 8 * i + 8, :] = x

    def row_copy(j, down):
        height = packed[j][2]
        if j == 0:
            span = pl.ds(0, 1)
            source = z_ref.at[distinct - 1 if down else 0, span]
        else:
            span = pl.ds(first_row[j], height)
            source = (below if down else above_ref).at[span]
        landing = up_in if down else down_in
        send(source, landing.at[span], piece_sem.at[j], (f_dn if down else f_up, tile, lev))

    def ship_near(j):
        row_copy(j, True)

        @pl.when(has_up)
        def _():
            row_copy(j, False)
        sent.pop()

    def ship_wrap(j):
        @pl.when(face == 0)
        def _():
            row_copy(j, False)

    def ship_rows(j):
        row_copy(j, True)
        row_copy(j, False)

    def pack_sides(j):
        start, count, packs = pieces[j]
        each = count // packs
        made = []
        for p in range(packs):
            made.append(pack_of(start + p * each, each // 8))
            pack[first_pack[j] + p] = made[-1]
        return made

    def ship_sides(j):
        span = pl.ds(first_pack[j], pieces[j][2])
        for landing, to in ((left_in, (face, t_rt, lev)), (right_in, (face, t_lf, lev))):
            if j == 0:
                send(pack.at[0, pl.ds(0, 1)], landing.at[0, pl.ds(0, 1)], side_sem.at[0], to)
            else:
                send(pack.at[span], landing.at[span], side_sem.at[j], to)

    source = [unit - 2, unit - 1, 0, 1]

    def pack_corners(which, made):
        for d in range(4):
            out = jnp.zeros((8, columns), f32)
            for p, value in enumerate(made):
                out = jnp.where(within == p, pltpu.roll(value, (p - source[d]) % columns, 1), out)
            if which:
                folded = pltpu.roll(pltpu.roll(out, 4, 0), unit // 2, 1)
                out = jnp.where(within < unit // 2, out, folded)
            corner[which, d] = out

    def corner_copy(which, d):
        part = pl.ds(0, 4 if which else 1)
        send(corner.at[which, d, part], corner_in.at[which, d, part],
             corner_sem.at[which], diagonals[d])

    def corners_known(which):
        corner_copy(which, 0)
        corner_copy(which, 1)

        @pl.when(has_up)
        def _():
            corner_copy(which, 2)
            corner_copy(which, 3)

    def corners_rest(which):
        @pl.when(face == 0)
        def _():
            corner_copy(which, 2)
            corner_copy(which, 3)
        del sent[-2:]

    def ship_corners(which):
        for d in range(4):
            corner_copy(which, d)

    east = [level_rows(wind.at[0], a) for a in range(rows)]
    north = [level_rows(wind.at[1], a) for a in range(rows)]
    speed, parts = None, []
    whole = max(c[1] for c in chunks)
    for a in range(rows):
        aa = jac[a] * (m[0][a] * east[a] + m[1][a] * north[a])
        bb = jac[a] * (m[2][a] * east[a] + m[3][a] * north[a])
        parts.append(((aa * w_col)[:levels], (bb * wr[a])[:levels]))
        spacing = jnp.sqrt(
            m[0][a] * m[0][a] + m[1][a] * m[1][a] + m[2][a] * m[2][a] + m[3][a] * m[3][a]
        )
        here = jnp.max(east[a] * east[a] + north[a] * north[a], axis=0, keepdims=True)
        here = jnp.sqrt(here) * spacing
        speed = here if speed is None else jnp.maximum(speed, here)

    @pl.when(face < nf)
    def _():
        for a, pair in enumerate(parts):
            for k in range(-(-whole // levels)):
                n = min(levels, whole - k * levels)
                a_ref[a, k * levels : k * levels + n, :] = pair[0][:n]
                b_ref[a, k * levels : k * levels + n, :] = pair[1][:n]

    def gathered(stage, base, count):
        best = peak[stage]
        if count:
            drain(2 * count, peak_sem.at[stage])
        for o in range(count):
            best = jnp.maximum(best, peak_in[base + o])
        return best

    def put_mass():
        whole_rows = lanes_plain(jnp.concatenate(
            [jnp.broadcast_to(x, (8, columns)) for x in merged(mass)], 0
        ))
        for r in range(distinct):
            put(0, 0, r, whole_rows[8 * r : 8 * r + 8])

    def tracers_of(k, wanted=tuple(range(distinct))):
        start, count, _ = chunks[k]
        q = [tracer[pl.ds(start * rows + a, count, stride=rows), :] for a in range(rows)]
        first = [q[a] * a_ref[a, :count, :] for a in range(rows)]
        x, y = {}, {}
        for a in range(rows):
            r = rep[a]
            if r in wanted:
                keep = mass[a] * q[a] - along_rows(first, a, step_d[a])
                second = q[a] * b_ref[a, :count, :]
                x[r], y[r] = (x[r] + keep, y[r] + second) if r in x else (keep, second)
        for r in wanted:
            put(pieces[k + 1][0], 0, r, lanes_both(x[r], y[r]))

    def ready(j):
        squeeze_rows(j)
        return pack_sides(j)

    traced[0].wait()
    insides, borders = tuple(range(1, distinct - 1)), (0, distinct - 1)
    tracers_of(0, borders)
    squeeze_rows(1)
    enter()
    ship_near(1)
    tracers_of(0, insides)
    made = pack_sides(1)
    ship_sides(1)

    drain(group_rows[1], in_sem.at[1])
    traced[1].wait()
    column_sums()
    put_mass()
    tracers_of(1)
    mass_made = pack_sides(0)
    pack_corners(0, mass_made)
    made += ready(2)
    ship_near(2)
    send_totals()
    ship_sides(2)
    ship_near(0)
    ship_sides(0)
    corners_known(0)

    drain(group_rows[3], in_sem.at[3])
    traced[2].wait()
    depth = [level_rows(thick, a) for a in range(rows)]
    depth_c = by_column(depth)
    flux_a, flux_b = [], []
    for a in range(rows):
        dr, dc = along_rows(depth, a, dd[a % 4]), depth_c[a]
        gx, gy = m[0][a] * dr + m[2][a] * dc, m[1][a] * dr + m[3][a] * dc
        flux_a.append(jac[a] * (m[0][a] * gx + m[1][a] * gy))
        flux_b.append(jac[a] * (m[2][a] * gx + m[3][a] * gy))
    flux_c = by_column(flux_b)
    damp = None
    for a in range(rows):
        lap = jnp.abs(along_rows(flux_a, a, dd[a % 4]) + flux_c[a])
        here = jnp.max(lap, axis=0, keepdims=True) / jac[a]
        damp = here if damp is None else jnp.maximum(damp, here)
    peak[0] = jnp.concatenate(
        [time_step * speed, (time_step * viscosity) * damp, jnp.zeros((6, columns), f32)], 0
    )
    tracers_of(2)
    made += ready(3)
    plane_meets()
    for o, peer in enumerate(plane):
        send(peak.at[0, pl.ds(0, 2)], peak_in.at[o, pl.ds(0, 2)], peak_sem.at[0], peer)
    ship_near(3)
    ship_sides(3)

    first, second, keep = [], [], []
    for a in range(rows):
        aa = jac[a] * (m[0][a] * east[a] + m[1][a] * north[a])
        bb = jac[a] * (m[2][a] * east[a] + m[3][a] * north[a])
        first.append(w_col * (depth[a] * aa - viscosity * flux_a[a]))
        second.append(wr[a] * (depth[a] * bb - viscosity * flux_b[a]))
    for a in range(rows):
        keep.append(mass[a] * depth[a] - along_rows(first, a, step_d[a]))
    for r, (x, y) in enumerate(zip(merged(keep), merged(second))):
        put(pieces[heat][0], pad, r, lanes_both(x, y))
    warm = [level_rows(temp, a) for a in range(rows)]
    warm_c = by_column(warm)
    value = []
    for a in range(rows):
        dr, dc = along_rows(warm, a, dd[a % 4]), warm_c[a]
        gx, gy = m[0][a] * dr + m[2][a] * dc, m[1][a] * dr + m[3][a] * dc
        value.append(mass[a] * (warm[a] - time_step * (east[a] * gx + north[a] * gy)))
    for r, x in enumerate(merged(value)):
        put(pieces[heat][0], 0, r, lanes_plain(x))
    made += ready(heat)
    pack_corners(1, made)
    corners_known(1)
    ship_near(heat)
    ship_sides(heat)

    traced[3].wait()
    tracers_of(3)
    later = ready(4)
    ends_meet()
    corners_rest(0)
    ship_near(4)
    ship_sides(4)
    corners_rest(1)
    for j in (0, 1, 2, 3, heat, 4):
        ship_wrap(j)

    if nl > 1:
        drain((nl - 1) * rows, total_sem.at[0])
    above = ground[...]
    for o in range(nl - 1):
        origin = lax.rem(lev + nl - (o + 1), nl)
        use = jnp.where(origin > lev, 1.0, 0.0).astype(f32)
        above = above + use * total_in[o]
    energy = []
    for a in range(rows):
        u, v = level_rows(wind.at[0], a), level_rows(wind.at[1], a)
        energy.append(0.5 * (u * u + v * v) + level_rows(geo, a) + above[a : a + 1, :])
    energy_c = by_column(energy)
    value_u, value_v = [], []
    for a in range(rows):
        u, v = level_rows(wind.at[0], a), level_rows(wind.at[1], a)
        dr, dc = along_rows(energy, a, dd[a % 4]), energy_c[a]
        value_u.append(mass[a] * (u - time_step * (m[0][a] * dr + m[2][a] * dc)))
        value_v.append(mass[a] * (v - time_step * (m[1][a] * dr + m[3][a] * dc)))
    for r, (x, y) in enumerate(zip(merged(value_u), merged(value_v))):
        put(pieces[last][0], 0, r, lanes_plain(x))
        put(pieces[last][0], pad, r, lanes_plain(y))
    later += ready(last)
    pack_corners(2, later)
    ship_corners(2)
    ship_rows(last)
    ship_sides(last)

    traced[4].wait()
    tracers_of(4)
    pack_corners(3, ready(5))
    ship_corners(3)
    ship_rows(5)
    ship_sides(5)
    for load in tables:
        load.wait()

    def seam(ref, f, t, k):
        return ref[f, k, t]

    codes = [
        lax.rem(4 - seam(rot_ref, f_up, tile, 0), 4), seam(rot_ref, face, tile, 0),
        lax.rem(4 - seam(rot_ref, face, t_lf, 1), 4), seam(rot_ref, face, tile, 1),
    ]
    flips = [
        seam(flip_ref, f_up, tile, 0), seam(flip_ref, face, tile, 0),
        seam(flip_ref, face, t_lf, 1), seam(flip_ref, face, tile, 1),
    ]
    tallies = [
        tally_ref[f_up, t_lf], tally_ref[f_up, tile],
        tally_ref[face, t_lf], tally_ref[face, tile],
    ]

    def cosine(code):
        return jnp.where(code == 0, 1.0, jnp.where(code == 2, -1.0, 0.0)).astype(f32)

    def sine(code):
        return jnp.where(code == 1, 1.0, jnp.where(code == 3, -1.0, 0.0)).astype(f32)

    def filled(x):
        return jnp.full((8, columns), x)

    odd = lax.rem(lane, 2) == 1
    mirror = lane - within + (unit - 2) - 2 * (within // 2) + lax.rem(within, 2)
    mirror = jnp.clip(mirror, 0, columns - 1)
    side_flip = jnp.where(odd, filled(flips[2]), filled(flips[3])) == 1
    side_cos = jnp.where(odd, filled(cosine(codes[2])), filled(cosine(codes[3])))
    side_sin = jnp.where(odd, filled(sine(codes[2])), filled(sine(codes[3])))
    corner_code = [
        lax.rem(codes[0] + codes[2], 4), lax.rem(codes[0] + codes[3], 4),
        lax.rem(codes[1] + codes[2], 4), lax.rem(codes[1] + codes[3], 4),
    ]
    target = [1, 0, unit - 1, unit - 2]
    alive = [filled(tallies[d]) == 4 for d in range(4)]

    def sides(index):
        if index == 0:
            a = jnp.broadcast_to(left_in[0, 0:1, :], (8, columns))
            b = jnp.broadcast_to(right_in[0, 0:1, :], (8, columns))
        else:
            a, b = left_in[index], right_in[index]
        x = jnp.where(odd, pltpu.roll(a, 1, 1), pltpu.roll(b, columns - 1, 1))
        return jnp.where(side_flip, jnp.take_along_axis(x, mirror, axis=1), x)

    def corner_tile(which, d):
        if which == 0:
            return jnp.broadcast_to(corner_in[0, d, 0:1, :], (8, columns))
        x = corner_in[which, d]
        lower = pltpu.roll(pltpu.roll(x, 4, 0), columns - unit // 2, 1)
        return jnp.where(sublane < 4, x, lower)

    def corner_values(which, d, p):
        x = corner_tile(which, d)
        x = pltpu.roll(x, (target[d] - p) % columns, 1)
        return jnp.where(alive[d] & (within == target[d]), x, 0.0)

    edge = (lane[:1] == 0) | (lane[:1] == columns - 1)

    def to_edges(x, i, r):
        y = pltpu.roll(x, (columns - (unit * i + 2 * r + 1)) % columns, 1)
        return jnp.where(edge, y, 0.0)

    rev = (columns - 1) - lane
    row_flip = [filled(flips[0]) == 1, filled(flips[1]) == 1]
    origin_lane = [jnp.where(row_flip[i], rev, lane) for i in range(2)]
    spread = [x - x // 4 for x in origin_lane]
    inner = [jnp.minimum(x, 3 * quarter - 1) for x in spread]
    rim_end = [x == columns - 1 for x in origin_lane]

    def row_rim(ref, which, j):
        if j == 0:
            x = jnp.broadcast_to(ref[0:1, :], (8, columns))
            return [jnp.take_along_axis(x, origin_lane[which], axis=1)]
        quads, width, _ = packed[j]
        at = first_row[j]
        got = [ref[at + 8 * i : at + 8 * i + 8, :] for i in range(width)]
        ends = got[-1]
        out = []
        for g in range(quads):
            one, two, three = got[3 * g : 3 * g + 3]
            four = jnp.where(
                lane < quarter, pltpu.roll(one, quarter, 1),
                jnp.where(lane < 2 * quarter, pltpu.roll(two, 2 * quarter, 1),
                          pltpu.roll(three, 3 * quarter, 1)),
            )
            for x in (one, two, three, four):
                spots = [p for p, _ in end_spots(j, len(out), x)]
                x = jnp.take_along_axis(x, inner[which], axis=1)
                parts = [jnp.broadcast_to(ends[:, p : p + 1], (8, columns)) for p in spots]
                end = parts[0]
                if len(parts) > 1:
                    end = jnp.where(sublane < 4, end, pltpu.roll(parts[1], 4, 0))
                out.append(jnp.where(rim_end[which], end, x))
        for x in got[3 * quads :]:
            out.append(jnp.take_along_axis(x, spread[which], axis=1))
        if j >= heat:
            second = pltpu.roll(out[-1], 8 - tail, 0)
            out = out[:full] + out[-1:] + out[full : 2 * full] + [second]
        return out

    sets = [[0], [1, 2, 3, heat], [4, last, last], [5]]
    corner_spot = {j: (w, group.index(j)) for w, group in enumerate(sets) for j in group}

    def sides_of(j):
        p = first_pack[j]
        if j < last:
            return [sides(p)]
        xu, xv = sides(p), sides(p + 1)
        return [side_cos * xu - side_sin * xv, side_sin * xu + side_cos * xv]

    def with_corners(j):
        which, p = corner_spot[j]
        if j < last:
            return [seam_x[first_pack[j]] + sum_corners(which, p)]
        xu, xv = seam_x[first_pack[j]], seam_x[first_pack[j] + 1]
        for d in range(4):
            cu, cv = corner_values(which, d, p), corner_values(which, d, p + 1)
            c, s = cosine(corner_code[d]), sine(corner_code[d])
            xu, xv = xu + (c * cu - s * cv), xv + (s * cu + c * cv)
        return [xu, xv]

    def sum_corners(which, p):
        parts = [corner_values(which, d, p) for d in range(4)]
        return parts[0] + parts[1] + parts[2] + parts[3]

    def rims_of(j):
        both = [row_rim(up_in, 0, j), row_rim(down_in, 1, j)]
        if j == last:
            for which in range(2):
                x = both[which]
                c, s = cosine(codes[which]), sine(codes[which])
                ru = [c * x[i] - s * x[groups + i] for i in range(groups)]
                rv = [s * x[i] + c * x[groups + i] for i in range(groups)]
                both[which] = ru + rv
        return both

    def stored(ref, begin, i, valid, r, x):
        n = min(8, valid - 8 * i)
        for a in range(rows):
            if rep[a] == r:
                ref[pl.ds((begin + 8 * i) * rows + a, n, stride=rows), :] = (x * inverse[a])[:n]

    inverse = [None] * rows

    def finish(j, seams, which_rows, both=None):
        start, total_count, packs = pieces[j]
        each = (total_count // packs) // 8
        for i in range(total_count // 8):
            for r in which_rows:
                x = z_ref[r, start + 8 * i : start + 8 * i + 8, :]
                x = x + to_edges(seams[i // each], i % each, r)
                if r in borders:
                    x = x + both[0 if r == 0 else 1][i]
                if j == 0:
                    for a in range(rows):
                        if rep[a] == r:
                            inverse[a] = 1.0 / x
                elif j < heat:
                    begin, _, valid = chunks[j - 1]
                    stored(tracer_o, begin, i, valid, r, x)
                else:
                    first_half, k = i < groups, i % groups
                    if j == heat:
                        ref = temp_o if first_half else thick_o
                    else:
                        ref = wind_o.at[0 if first_half else 1]
                    stored(ref, 0, k, levels, r, x)

    groups = pad // 8
    def finish_insides(order):
        for j in order:
            drain(2 * side_rows[j], side_sem.at[j])
        for j in order:
            seams = sides_of(j)
            for i, x in enumerate(seams):
                seam_x[first_pack[j] + i] = x
            finish(j, seams, insides)

    def finish_borders(order, corners):
        for j in order:
            drain(2 * packed[j][2], piece_sem.at[j])
        for which in corners:
            drain(16 if which else 4, corner_sem.at[which])
        for j in order:
            finish(j, with_corners(j), borders, rims_of(j))

    finish_insides([0, 1, 2, 3, heat, 4])
    peak[1] = gathered(0, 0, len(plane))
    for o in range(1, nf):
        send(peak.at[1, pl.ds(0, 2)], peak_in.at[len(plane) + o - 1, pl.ds(0, 2)],
             peak_sem.at[1], (lax.rem(face + o, nf), tile, lev))
    finish_borders([0, 1, 2, 3, heat], [0, 1])
    finish_insides([last, 5])
    finish_borders([4, last], [2])
    finish_borders([5], [3])

    bound_o[...] = gathered(1, len(plane), nf - 1)
    drain(sum(sent), sent_sem.at[0])


def write_out(wind, temp, thick, tracer, bound, wind_o, temp_o, thick_o, tracer_o, bound_o, sem):
    pairs = ((tracer, tracer_o), (wind, wind_o), (temp, temp_o), (thick, thick_o))
    copies = [pltpu.make_async_copy(a, b, sem.at[i]) for i, (a, b) in enumerate(pairs)]
    for copy in copies:
        copy.start()
    bound_o[0] = jnp.max(bound[0:1, :])
    bound_o[1] = jnp.max(bound[1:2, :])
    for copy in copies:
        copy.wait()


def on_device(
    sizes, wind, temp, thick, tracers, ground, maps, det, rot, flip, tally
):
    nf, nt, nl = sizes
    levels, rows, columns = temp.shape
    count = tracers.shape[0]
    chunks = layout(levels, count)
    pad = -(-levels // 8) * 8
    if rows != 8 or columns != 128 or levels % 8 not in (1, 2, 3, 4) or len(chunks) != 5:
        raise ValueError("block shape")
    table, dct, w_col = lane_tables(columns)
    distinct = rows - rows // 4 + 1
    total_rows = 4 * pad + 8 + sum(c[1] for c in chunks)
    pieces = len(chunks) + 3
    packs = len(chunks) + 4
    landing = sum(8 * p[1] for p in packing(levels, chunks))
    whole = max(c[1] for c in chunks)
    n = levels * rows
    dma = pltpu.SemaphoreType.DMA
    peers = nt * nl - 1 + nf - 1
    hbm = pl.BlockSpec(memory_space=pl.ANY)
    smem = pl.BlockSpec(memory_space=pltpu.SMEM)
    vmem = pl.BlockSpec(memory_space=pltpu.VMEM)
    last = chunks[-1]
    shapes = ((2, n, columns), (n, columns), (n, columns), (count * n, columns), (8, columns))
    outs = pl.pallas_call(
        functools.partial(kernel, sizes, (levels, rows, columns, chunks, pad)),
        out_shape=tuple(pltpu.VMEM(shape, f32) for shape in shapes),
        in_specs=[hbm] * 13,
        out_specs=(vmem,) * 5,
        scratch_shapes=[
            pltpu.VMEM((2, pad * rows, columns), f32),
            pltpu.VMEM((pad * rows, columns), f32),
            pltpu.VMEM((pad * rows, columns), f32),
            pltpu.VMEM(((last[0] + last[1]) * rows, columns), f32),
            pltpu.VMEM((pad * rows, columns), f32),
            pltpu.VMEM((rows, columns), f32),
            pltpu.VMEM((4 * rows, columns), f32),
            pltpu.VMEM((rows, columns), f32),
            pltpu.VMEM(table.shape, bf16),
            pltpu.VMEM(dct.shape, bf16),
            pltpu.VMEM((1, columns), f32),
            pltpu.VMEM((rows, whole, columns), f32),
            pltpu.VMEM((rows, whole, columns), f32),
            pltpu.VMEM((distinct, total_rows, columns), f32),
            pltpu.VMEM((landing, columns), f32),
            pltpu.VMEM((landing, columns), f32),
            pltpu.VMEM((packs, 8, columns), f32),
            pltpu.VMEM((packs, 8, columns), f32),
            pltpu.VMEM((4, 4, 8, columns), f32),
            pltpu.VMEM((rows, columns), f32),
            pltpu.VMEM((3, 8, columns), f32),
            pltpu.VMEM((landing, columns), f32),
            pltpu.VMEM((landing, columns), f32),
            pltpu.VMEM((packs, 8, columns), f32),
            pltpu.VMEM((packs, 8, columns), f32),
            pltpu.VMEM((4, 4, 8, columns), f32),
            pltpu.VMEM((nl - 1, rows, columns), f32),
            pltpu.VMEM((peers, 8, columns), f32),
            pltpu.SMEM((nf, 2, nt), jnp.int32),
            pltpu.SMEM((nf, 2, nt), jnp.int32),
            pltpu.SMEM((nf, nt), jnp.int32),
            dma((7 + len(chunks),)),
            dma((1,)),
            dma((pieces,)),
            dma((pieces,)),
            dma((4,)),
            dma((1,)),
            dma((3,)),
            pltpu.SemaphoreType.REGULAR((2,)),
        ],
        compiler_params=pltpu.CompilerParams(collective_id=0, has_side_effects=True),
    )(
        wind.reshape(2, n, columns), temp.reshape(n, columns), thick.reshape(n, columns),
        tracers.reshape(count * n, columns), ground, maps.reshape(4 * rows, columns), det,
        table, dct, w_col, rot.transpose(0, 2, 1), flip.transpose(0, 2, 1), tally,
    )
    outs = pl.pallas_call(
        write_out,
        out_shape=tuple(jax.ShapeDtypeStruct(x, f32) for x in shapes[:4] + ((2,),)),
        in_specs=[vmem] * 5,
        out_specs=(hbm,) * 4 + (smem,),
        scratch_shapes=[dma((4,))],
    )(*[pltpu.with_memory_space_constraint(x, pltpu.VMEM) for x in outs])
    return (
        outs[0].reshape(wind.shape), outs[1].reshape(temp.shape), outs[2].reshape(thick.shape),
        outs[3].reshape(tracers.shape), outs[4],
    )


def solution(mesh):
    sizes = tuple(mesh.shape[name] for name in ("face", "tile", "lev"))
    level = P("lev", "face", "tile")
    stacked = P(None, "lev", "face", "tile")
    return jax.shard_map(
        functools.partial(on_device, sizes),
        mesh=mesh,
        in_specs=(stacked, level, level, stacked, P("face", "tile"), P(None, "face", "tile"),
                  P("face", "tile"), P(), P(), P()),
        out_specs=(stacked, level, level, stacked, P()),
        check_vma=False,
    )
```

```python
import functools
import math

import jax
import jax.numpy as jnp
import numpy as np
from jax import lax
from jax.experimental import pallas as pl
from jax.experimental.pallas import tpu as pltpu
from jax.sharding import PartitionSpec as P

time_step = 0.05
viscosity = 0.05
f32 = jnp.float32
bf16 = jnp.bfloat16
MESH = pl.DeviceIdType.MESH
highest = lax.Precision.HIGHEST


def gll_tables():
    offset = 1.0 / math.sqrt(5.0)
    nodes = np.array([-1.0, -offset, offset, 1.0])
    weights = np.array([1.0 / 6.0, 5.0 / 6.0, 5.0 / 6.0, 1.0 / 6.0])
    bary = np.ones(4)
    for i in range(4):
        for j in range(4):
            if j != i:
                bary[i] = bary[i] / (nodes[i] - nodes[j])
    derivative = np.zeros((4, 4))
    for i in range(4):
        for j in range(4):
            if j != i:
                derivative[i, j] = bary[j] / bary[i] / (nodes[i] - nodes[j])
        derivative[i, i] = -np.sum(derivative[i])
    return derivative, weights


def lane_tables(columns):
    derivative, weights = gll_tables()
    d = np.kron(np.eye(columns // 4), derivative)
    s = np.eye(columns)
    for c in range(columns - 1):
        if c % 4 == 3:
            s[c, c + 1] = s[c + 1, c] = 1.0
    w = np.tile(weights, columns // 4)
    t = (-time_step * (d.T * w[None, :]) @ s).astype(np.float32)
    t_hi = jnp.asarray(t).astype(bf16)
    t_lo = (jnp.asarray(t) - t_hi.astype(f32)).astype(bf16)
    sb = jnp.asarray(s, bf16)
    d_t = jnp.asarray(d.T, f32)
    d_hi = d_t.astype(bf16)
    d_lo = (d_t - d_hi.astype(f32)).astype(bf16)
    return jnp.concatenate([sb, sb, t_hi, t_hi, t_lo], 0), jnp.concatenate([d_hi, d_hi, d_lo], 0), jnp.asarray(w[None, :], f32)


def split(x):
    hi = x.astype(bf16)
    return hi, (x - hi.astype(f32)).astype(bf16)


def layout(levels, tracers):
    group = 8 // math.gcd(levels, 8)
    chunks, q = [], 0
    while q < tracers:
        n = min(group, tracers - q)
        chunks.append((q * levels, -(-n * levels // 8) * 8, n * levels))
        q += n
    return chunks


def packing(levels, chunks):
    sizes = [(c[1] // 8, c[2] - (c[1] - 8)) for c in chunks]
    sizes += [(2 * (levels // 8) + 1, 2 * (levels % 8))] * 2
    out = [(0, 1, 1)]
    for tiles, left in sizes:
        quads = (tiles - 1) // 4
        width = tiles - quads
        out.append((quads, width, 8 * width - (4 if left <= 4 else 0)))
    return out


def kernel(
    sizes, dims,
    wind_h, temp_h, thick_h, tracer_h, ground_h, maps_h, det_h, ops_h, dct_h, wc_h,
    rot_h, flip_h, tally_h,
    wind_o, temp_o, thick_o, tracer_o, bound_o,
    wind, temp, thick, tracer, geo, ground, maps, det, ops, dct, wc,
    a_ref, b_ref, z_ref, below, above_ref, pack, seam_x, corner, total, peak,
    up_in, down_in, left_in, right_in, corner_in, total_in, peak_in,
    rot_ref, flip_ref, tally_ref,
    in_sem, sent_sem, piece_sem, side_sem, corner_sem, total_sem, peak_sem, chain_sem,
):
    nf, nt, nl = sizes
    levels, rows, columns, chunks, pad = dims
    derivative, weights = gll_tables()
    rep = [a - (a // 4) for a in range(rows)]
    distinct = rows - rows // 4 + 1
    face, tile, lev = lax.axis_index("face"), lax.axis_index("tile"), lax.axis_index("lev")
    f_up, f_dn = lax.rem(face + nf - 1, nf), lax.rem(face + 1, nf)
    t_lf, t_rt = lax.rem(tile + nt - 1, nt), lax.rem(tile + 1, nt)

    pieces = [(0, 8, 1)]
    at = 8
    for _, count, _ in chunks:
        pieces.append((at, count, 1))
        at += count
    pieces.append((at, 2 * pad, 1))
    pieces.append((at + 2 * pad, 2 * pad, 2))
    first_pack = np.cumsum([0] + [p[2] for p in pieces]).tolist()
    last = len(pieces) - 1
    heat = last - 1
    full, tail = levels // 8, levels % 8
    packed = packing(levels, chunks)
    first_row = np.cumsum([0] + [8 * p[1] for p in packed]).tolist()
    quarter = columns // 4
    side_rows = [1] + [8 * p[2] for p in pieces[1:]]

    n = levels * rows
    groups_in = [
        [(maps_h, maps), (det_h, det), (wc_h, wc),
         (wind_h.at[0], wind.at[0, :n]), (wind_h.at[1], wind.at[1, :n])],
        [(temp_h, temp.at[:n]), (thick_h, thick.at[:n])],
        [(ops_h, ops)],
        [(dct_h, dct), (ground_h, ground)],
    ]
    group_rows = [5 * rows + 1 + 2 * n, 2 * n, 5 * columns // 2, 3 * columns // 2 + rows]
    n0 = len(groups_in)
    spans = [pl.ds(start * rows, valid * rows) for start, _, valid in chunks]
    traced = [
        pltpu.make_async_copy(tracer_h.at[span], tracer.at[span], in_sem.at[n0 + k])
        for k, span in enumerate(spans)
    ]
    tables = [(rot_h, rot_ref), (flip_h, flip_ref), (tally_h, tally_ref)]
    at = n0 + len(chunks)
    tables = [pltpu.make_async_copy(s, d, in_sem.at[at + i]) for i, (s, d) in enumerate(tables)]

    def fetch(i):
        for s, d in groups_in[i]:
            pltpu.make_async_copy(s, d, in_sem.at[i]).start()

    def drain(count, sem):
        view = z_ref.at[0, pl.ds(0, count)] if count <= z_ref.shape[1] else tracer.at[pl.ds(0, count)]
        pltpu.make_async_copy(view, view, sem).wait()

    fetch(0)
    traced[0].start()
    fetch(2)
    fetch(1)
    for load in traced[1:]:
        load.start()
    fetch(3)
    for load in tables:
        load.start()

    diagonals = [(f_dn, t_rt, lev), (f_dn, t_lf, lev), (f_up, t_rt, lev), (f_up, t_lf, lev)]
    barrier = pltpu.get_barrier_semaphore()

    def notify(sem, to):
        pl.semaphore_signal(sem, inc=1, device_id=to, device_id_type=MESH)

    has_up, has_dn = face > 0, face < nf - 1
    at_end = face == nf - 1
    plane = [
        (face, lax.rem(tile + o, nt), lax.rem(lev + p, nl))
        for o in range(nt) for p in range(nl) if o or p
    ]

    def one(flag):
        return jnp.where(flag, 1, 0)

    for o in range(nf - 1, 1, -1):
        @pl.when(face + o < nf)
        def _():
            notify(barrier, (face + o, tile, lev))
    for here, other in ((has_up, face - 1), (has_dn, face + 1)):
        @pl.when(here)
        def _():
            for t in (tile, t_lf, t_rt):
                notify(barrier, (other, t, lev))

    @pl.when(face == 0)
    def _():
        for t in (t_lf, t_rt):
            notify(barrier, (nf - 1, t, lev))
    for o in range(nt):
        for p in range(nl):
            if o and p:
                @pl.when(tile + o < nt)
                def _():
                    notify(barrier, (face, tile + o, lax.rem(lev + p, nl)))
            elif o or p:
                notify(barrier, (face, lax.rem(tile + o, nt), lax.rem(lev + p, nl)))
    known = (
        nt - 1 + (nl - 1) * (1 + tile) + face + one(has_dn)
        + 2 * (one(has_up) + one(has_dn) + one(at_end))
    )
    unknown = jnp.maximum(nf - 2 - face, 0) + 2 * one(face == 0)
    beside = (nt - 1 - tile) * (nl - 1)

    def enter():
        pl.semaphore_wait(barrier, known)
        for o in range(2, nf):
            @pl.when(face - o >= 0)
            def _():
                notify(chain_sem.at[0], (face - o, tile, lev))

        @pl.when(at_end)
        def _():
            for t in (t_lf, t_rt):
                notify(chain_sem.at[0], (0, t, lev))
        for o in range(1, nt):
            for p in range(1, nl):
                @pl.when(tile - o >= 0)
                def _():
                    notify(chain_sem.at[1], (face, tile - o, lax.rem(lev + p, nl)))

    def plane_meets():
        @pl.when(beside > 0)
        def _():
            pl.semaphore_wait(chain_sem.at[1], beside)

    def ends_meet():
        @pl.when(unknown > 0)
        def _():
            pl.semaphore_wait(chain_sem.at[0], unknown)

    extra = (pad - levels) * rows
    if extra:
        zero = jnp.zeros((extra, columns), f32)
        temp[levels * rows :, :] = zero
        thick[levels * rows :, :] = zero
        geo[levels * rows :, :] = zero
        wind[0, levels * rows :, :] = zero
        wind[1, levels * rows :, :] = zero
    end = chunks[-1][0] + chunks[-1][2]
    more = chunks[-1][1] - chunks[-1][2]
    if more:
        tracer[end * rows :, :] = jnp.zeros((more * rows, columns), f32)

    sent = []

    def send(src, dst, r, to):
        pltpu.make_async_remote_copy(
            src_ref=src, dst_ref=dst, send_sem=sent_sem.at[0], recv_sem=r,
            device_id=to, device_id_type=MESH,
        ).start()
        sent.append(math.prod(src.shape) // columns)

    def column_sums():
        acc = jnp.zeros((rows, columns), f32)
        for k in reversed(range(levels)):
            term = temp[k * rows : (k + 1) * rows, :] * thick[k * rows : (k + 1) * rows, :]
            geo[k * rows : (k + 1) * rows, :] = acc + 0.5 * term
            acc = acc + term
        total[...] = acc

    def send_totals():
        for o in range(1, nl):
            send(total, total_in.at[o - 1], total_sem.at[0], (face, tile, lax.rem(lev + o, nl)))

    drain(group_rows[0], in_sem.at[0])
    w_col = wc[...]
    drain(group_rows[2], in_sem.at[2])
    table = ops[...]
    narrow = ops[: 2 * columns, :]
    wr = [float(weights[a % 4]) for a in range(rows)]
    m = [[maps[e * rows + a : e * rows + a + 1, :] for a in range(rows)] for e in range(4)]
    jac = [det[a : a + 1, :] for a in range(rows)]
    mass = [jac[a] * (wr[a] * w_col) for a in range(rows)]
    step_d = [[float(time_step * wr[a] * derivative[a % 4, b]) for b in range(4)] for a in range(rows)]
    dd = [[float(derivative[i, j]) for j in range(4)] for i in range(4)]

    def level_rows(ref, a):
        return ref[pl.ds(a, pad, stride=rows), :]

    def along_rows(values, a, coef):
        base = a - a % 4
        out = coef[0] * values[base]
        for b in range(1, 4):
            out = out + coef[b] * values[base + b]
        return out

    def merged(values):
        out = [None] * distinct
        for a in range(rows):
            r = rep[a]
            out[r] = values[a] if out[r] is None else out[r] + values[a]
        return out

    def lanes_plain(x):
        hi, lo = split(x)
        return jnp.dot(jnp.concatenate([hi, lo], 1), narrow, preferred_element_type=f32)

    def lanes_both(p, g):
        ph, plo = split(p)
        gh, glo = split(g)
        return jnp.dot(
            jnp.concatenate([ph, plo, gh, glo, gh], 1), table, preferred_element_type=f32
        )

    def by_column(values):
        stacked = jnp.concatenate(values, 0)
        hi, lo = split(stacked)
        out = jnp.dot(
            jnp.concatenate([hi, lo, hi], 1), dct[...], preferred_element_type=f32
        )
        n = values[0].shape[0]
        return [out[i * n : (i + 1) * n] for i in range(len(values))]

    lane = lax.broadcasted_iota(jnp.int32, (8, columns), 1)
    unit = 2 * distinct
    within = lax.rem(lane, unit)

    def put(piece, offset, r, z):
        z_ref[r, piece + offset : piece + offset + z.shape[0], :] = z

    def pack_of(start, groups):
        out = jnp.zeros((8, columns), f32)
        for i in range(groups):
            for r in range(distinct):
                spot = unit * i + 2 * r
                value = pltpu.roll(z_ref[r, start + 8 * i : start + 8 * i + 8, :], spot + 1, 1)
                out = jnp.where((lane == spot) | (lane == spot + 1), value, out)
        return out

    squeeze = jnp.minimum(lane + lane // 3, columns - 1)
    sublane = lax.broadcasted_iota(jnp.int32, (8, columns), 0)

    def tiles_of(j, r):
        start, count, _ = pieces[j]

        def tile_at(row):
            return z_ref[r, row : row + 8, :]

        if j < heat:
            return [tile_at(start + 8 * i) for i in range(count // 8)]
        out = [tile_at(start + half + 8 * i) for half in (0, pad) for i in range(full)]
        second = pltpu.roll(tile_at(start + pad + 8 * full), tail, 0)
        return out + [jnp.where(sublane < tail, tile_at(start + 8 * full), second)]

    def end_spots(j, i, x):
        spot = 3 * quarter + 1
        if packed[j][2] % 8 == 0:
            return [(spot + i, x)]
        return [(spot + 2 * i, x), (spot + 2 * i + 1, pltpu.roll(x, 4, 0))]

    def squeeze_rows(j):
        quads = packed[j][0]
        at = first_row[j]
        for r, out in ((distinct - 1, below), (0, above_ref)):
            wide = tiles_of(j, r)
            thin = [jnp.take_along_axis(x, squeeze, axis=1) for x in wide]
            done = []
            for g in range(quads):
                spare = thin[4 * g + 3]
                for t in range(3):
                    done.append(jnp.where(
                        lane < 3 * quarter, thin[4 * g + t],
                        pltpu.roll(spare, (3 - t) * quarter, 1),
                    ))
            done += thin[4 * quads :]
            for i in range(4 * quads):
                for spot, x in end_spots(j, i, wide[i]):
                    done[-1] = jnp.where(
                        lane == spot, pltpu.roll(x, (spot + 1) % columns, 1), done[-1]
                    )
            for i, x in enumerate(done):
                out[at + 8 * i : at + 8 * i + 8, :] = x

    def row_copy(j, down):
        height = packed[j][2]
        if j == 0:
            span = pl.ds(0, 1)
            source = z_ref.at[distinct - 1 if down else 0, span]
        else:
            span = pl.ds(first_row[j], height)
            source = (below if down else above_ref).at[span]
        landing = up_in if down else down_in
        send(source, landing.at[span], piece_sem.at[j], (f_dn if down else f_up, tile, lev))

    def ship_near(j):
        row_copy(j, True)

        @pl.when(has_up)
        def _():
            row_copy(j, False)
        sent.pop()

    def ship_wrap(j):
        @pl.when(face == 0)
        def _():
            row_copy(j, False)

    def ship_rows(j):
        row_copy(j, True)
        row_copy(j, False)

    def pack_sides(j):
        start, count, packs = pieces[j]
        each = count // packs
        made = []
        for p in range(packs):
            made.append(pack_of(start + p * each, each // 8))
            pack[first_pack[j] + p] = made[-1]
        return made

    def ship_sides(j):
        span = pl.ds(first_pack[j], pieces[j][2])
        for landing, to in ((left_in, (face, t_rt, lev)), (right_in, (face, t_lf, lev))):
            if j == 0:
                send(pack.at[0, pl.ds(0, 1)], landing.at[0, pl.ds(0, 1)], side_sem.at[0], to)
            else:
                send(pack.at[span], landing.at[span], side_sem.at[j], to)

    source = [unit - 2, unit - 1, 0, 1]

    def pack_corners(which, made):
        for d in range(4):
            out = jnp.zeros((8, columns), f32)
            for p, value in enumerate(made):
                out = jnp.where(within == p, pltpu.roll(value, (p - source[d]) % columns, 1), out)
            if which:
                folded = pltpu.roll(pltpu.roll(out, 4, 0), unit // 2, 1)
                out = jnp.where(within < unit // 2, out, folded)
            corner[which, d] = out

    def corner_copy(which, d):
        part = pl.ds(0, 4 if which else 1)
        send(corner.at[which, d, part], corner_in.at[which, d, part],
             corner_sem.at[which], diagonals[d])

    def corners_known(which):
        corner_copy(which, 0)
        corner_copy(which, 1)

        @pl.when(has_up)
        def _():
            corner_copy(which, 2)
            corner_copy(which, 3)

    def corners_rest(which):
        @pl.when(face == 0)
        def _():
            corner_copy(which, 2)
            corner_copy(which, 3)
        del sent[-2:]

    def ship_corners(which):
        for d in range(4):
            corner_copy(which, d)

    east = [level_rows(wind.at[0], a) for a in range(rows)]
    north = [level_rows(wind.at[1], a) for a in range(rows)]
    speed, parts = None, []
    whole = max(c[1] for c in chunks)
    for a in range(rows):
        aa = jac[a] * (m[0][a] * east[a] + m[1][a] * north[a])
        bb = jac[a] * (m[2][a] * east[a] + m[3][a] * north[a])
        parts.append(((aa * w_col)[:levels], (bb * wr[a])[:levels]))
        spacing = jnp.sqrt(
            m[0][a] * m[0][a] + m[1][a] * m[1][a] + m[2][a] * m[2][a] + m[3][a] * m[3][a]
        )
        here = jnp.max(east[a] * east[a] + north[a] * north[a], axis=0, keepdims=True)
        here = jnp.sqrt(here) * spacing
        speed = here if speed is None else jnp.maximum(speed, here)

    @pl.when(face < nf)
    def _():
        for a, pair in enumerate(parts):
            for k in range(-(-whole // levels)):
                n = min(levels, whole - k * levels)
                a_ref[a, k * levels : k * levels + n, :] = pair[0][:n]
                b_ref[a, k * levels : k * levels + n, :] = pair[1][:n]

    def gathered(stage, base, count):
        best = peak[stage]
        if count:
            drain(2 * count, peak_sem.at[stage])
        for o in range(count):
            best = jnp.maximum(best, peak_in[base + o])
        return best

    def put_mass():
        whole_rows = lanes_plain(jnp.concatenate(
            [jnp.broadcast_to(x, (8, columns)) for x in merged(mass)], 0
        ))
        for r in range(distinct):
            put(0, 0, r, whole_rows[8 * r : 8 * r + 8])

    def tracers_of(k, wanted=tuple(range(distinct))):
        start, count, _ = chunks[k]
        q = [tracer[pl.ds(start * rows + a, count, stride=rows), :] for a in range(rows)]
        first = [q[a] * a_ref[a, :count, :] for a in range(rows)]
        x, y = {}, {}
        for a in range(rows):
            r = rep[a]
            if r in wanted:
                keep = mass[a] * q[a] - along_rows(first, a, step_d[a])
                second = q[a] * b_ref[a, :count, :]
                x[r], y[r] = (x[r] + keep, y[r] + second) if r in x else (keep, second)
        for r in wanted:
            put(pieces[k + 1][0], 0, r, lanes_both(x[r], y[r]))

    def ready(j):
        squeeze_rows(j)
        return pack_sides(j)

    traced[0].wait()
    insides, borders = tuple(range(1, distinct - 1)), (0, distinct - 1)
    tracers_of(0, borders)
    squeeze_rows(1)
    enter()
    ship_near(1)
    tracers_of(0, insides)
    made = pack_sides(1)
    ship_sides(1)

    drain(group_rows[1], in_sem.at[1])
    traced[1].wait()
    column_sums()
    put_mass()
    tracers_of(1)
    mass_made = pack_sides(0)
    pack_corners(0, mass_made)
    made += ready(2)
    ship_near(2)
    send_totals()
    ship_sides(2)
    ship_near(0)
    ship_sides(0)
    corners_known(0)

    drain(group_rows[3], in_sem.at[3])
    traced[2].wait()
    depth = [level_rows(thick, a) for a in range(rows)]
    depth_c = by_column(depth)
    flux_a, flux_b = [], []
    for a in range(rows):
        dr, dc = along_rows(depth, a, dd[a % 4]), depth_c[a]
        gx, gy = m[0][a] * dr + m[2][a] * dc, m[1][a] * dr + m[3][a] * dc
        flux_a.append(jac[a] * (m[0][a] * gx + m[1][a] * gy))
        flux_b.append(jac[a] * (m[2][a] * gx + m[3][a] * gy))
    flux_c = by_column(flux_b)
    damp = None
    for a in range(rows):
        lap = jnp.abs(along_rows(flux_a, a, dd[a % 4]) + flux_c[a])
        here = jnp.max(lap, axis=0, keepdims=True) / jac[a]
        damp = here if damp is None else jnp.maximum(damp, here)
    peak[0] = jnp.concatenate(
        [time_step * speed, (time_step * viscosity) * damp, jnp.zeros((6, columns), f32)], 0
    )
    tracers_of(2)
    made += ready(3)
    plane_meets()
    for o, peer in enumerate(plane):
        send(peak.at[0, pl.ds(0, 2)], peak_in.at[o, pl.ds(0, 2)], peak_sem.at[0], peer)
    ship_near(3)
    ship_sides(3)

    first, second, keep = [], [], []
    for a in range(rows):
        aa = jac[a] * (m[0][a] * east[a] + m[1][a] * north[a])
        bb = jac[a] * (m[2][a] * east[a] + m[3][a] * north[a])
        first.append(w_col * (depth[a] * aa - viscosity * flux_a[a]))
        second.append(wr[a] * (depth[a] * bb - viscosity * flux_b[a]))
    for a in range(rows):
        keep.append(mass[a] * depth[a] - along_rows(first, a, step_d[a]))
    for r, (x, y) in enumerate(zip(merged(keep), merged(second))):
        put(pieces[heat][0], pad, r, lanes_both(x, y))
    warm = [level_rows(temp, a) for a in range(rows)]
    warm_c = by_column(warm)
    value = []
    for a in range(rows):
        dr, dc = along_rows(warm, a, dd[a % 4]), warm_c[a]
        gx, gy = m[0][a] * dr + m[2][a] * dc, m[1][a] * dr + m[3][a] * dc
        value.append(mass[a] * (warm[a] - time_step * (east[a] * gx + north[a] * gy)))
    for r, x in enumerate(merged(value)):
        put(pieces[heat][0], 0, r, lanes_plain(x))
    made += ready(heat)
    pack_corners(1, made)
    corners_known(1)
    ship_near(heat)
    ship_sides(heat)

    traced[3].wait()
    tracers_of(3)
    later = ready(4)
    ends_meet()
    corners_rest(0)
    ship_near(4)
    ship_sides(4)
    corners_rest(1)
    for j in (0, 1, 2, 3, heat, 4):
        ship_wrap(j)

    if nl > 1:
        drain((nl - 1) * rows, total_sem.at[0])
    above = ground[...]
    for o in range(nl - 1):
        origin = lax.rem(lev + nl - (o + 1), nl)
        use = jnp.where(origin > lev, 1.0, 0.0).astype(f32)
        above = above + use * total_in[o]
    energy = []
    for a in range(rows):
        u, v = level_rows(wind.at[0], a), level_rows(wind.at[1], a)
        energy.append(0.5 * (u * u + v * v) + level_rows(geo, a) + above[a : a + 1, :])
    energy_c = by_column(energy)
    value_u, value_v = [], []
    for a in range(rows):
        u, v = level_rows(wind.at[0], a), level_rows(wind.at[1], a)
        dr, dc = along_rows(energy, a, dd[a % 4]), energy_c[a]
        value_u.append(mass[a] * (u - time_step * (m[0][a] * dr + m[2][a] * dc)))
        value_v.append(mass[a] * (v - time_step * (m[1][a] * dr + m[3][a] * dc)))
    for r, (x, y) in enumerate(zip(merged(value_u), merged(value_v))):
        put(pieces[last][0], 0, r, lanes_plain(x))
        put(pieces[last][0], pad, r, lanes_plain(y))
    later += ready(last)
    pack_corners(2, later)
    ship_corners(2)
    ship_rows(last)
    ship_sides(last)

    traced[4].wait()
    tracers_of(4)
    pack_corners(3, ready(5))
    ship_corners(3)
    ship_rows(5)
    ship_sides(5)
    for load in tables:
        load.wait()

    def seam(ref, f, t, k):
        return ref[f, k, t]

    codes = [
        lax.rem(4 - seam(rot_ref, f_up, tile, 0), 4), seam(rot_ref, face, tile, 0),
        lax.rem(4 - seam(rot_ref, face, t_lf, 1), 4), seam(rot_ref, face, tile, 1),
    ]
    flips = [
        seam(flip_ref, f_up, tile, 0), seam(flip_ref, face, tile, 0),
        seam(flip_ref, face, t_lf, 1), seam(flip_ref, face, tile, 1),
    ]
    tallies = [
        tally_ref[f_up, t_lf], tally_ref[f_up, tile],
        tally_ref[face, t_lf], tally_ref[face, tile],
    ]

    def cosine(code):
        return jnp.where(code == 0, 1.0, jnp.where(code == 2, -1.0, 0.0)).astype(f32)

    def sine(code):
        return jnp.where(code == 1, 1.0, jnp.where(code == 3, -1.0, 0.0)).astype(f32)

    def filled(x):
        return jnp.full((8, columns), x)

    odd = lax.rem(lane, 2) == 1
    mirror = lane - within + (unit - 2) - 2 * (within // 2) + lax.rem(within, 2)
    mirror = jnp.clip(mirror, 0, columns - 1)
    side_flip = jnp.where(odd, filled(flips[2]), filled(flips[3])) == 1
    side_cos = jnp.where(odd, filled(cosine(codes[2])), filled(cosine(codes[3])))
    side_sin = jnp.where(odd, filled(sine(codes[2])), filled(sine(codes[3])))
    corner_code = [
        lax.rem(codes[0] + codes[2], 4), lax.rem(codes[0] + codes[3], 4),
        lax.rem(codes[1] + codes[2], 4), lax.rem(codes[1] + codes[3], 4),
    ]
    target = [1, 0, unit - 1, unit - 2]
    alive = [filled(tallies[d]) == 4 for d in range(4)]

    def sides(index):
        if index == 0:
            a = jnp.broadcast_to(left_in[0, 0:1, :], (8, columns))
            b = jnp.broadcast_to(right_in[0, 0:1, :], (8, columns))
        else:
            a, b = left_in[index], right_in[index]
        x = jnp.where(odd, pltpu.roll(a, 1, 1), pltpu.roll(b, columns - 1, 1))
        return jnp.where(side_flip, jnp.take_along_axis(x, mirror, axis=1), x)

    def corner_tile(which, d):
        if which == 0:
            return jnp.broadcast_to(corner_in[0, d, 0:1, :], (8, columns))
        x = corner_in[which, d]
        lower = pltpu.roll(pltpu.roll(x, 4, 0), columns - unit // 2, 1)
        return jnp.where(sublane < 4, x, lower)

    def corner_values(which, d, p):
        x = corner_tile(which, d)
        x = pltpu.roll(x, (target[d] - p) % columns, 1)
        return jnp.where(alive[d] & (within == target[d]), x, 0.0)

    edge = (lane[:1] == 0) | (lane[:1] == columns - 1)

    def to_edges(x, i, r):
        y = pltpu.roll(x, (columns - (unit * i + 2 * r + 1)) % columns, 1)
        return jnp.where(edge, y, 0.0)

    rev = (columns - 1) - lane
    row_flip = [filled(flips[0]) == 1, filled(flips[1]) == 1]
    origin_lane = [jnp.where(row_flip[i], rev, lane) for i in range(2)]
    spread = [x - x // 4 for x in origin_lane]
    inner = [jnp.minimum(x, 3 * quarter - 1) for x in spread]
    rim_end = [x == columns - 1 for x in origin_lane]

    def row_rim(ref, which, j):
        if j == 0:
            x = jnp.broadcast_to(ref[0:1, :], (8, columns))
            return [jnp.take_along_axis(x, origin_lane[which], axis=1)]
        quads, width, _ = packed[j]
        at = first_row[j]
        got = [ref[at + 8 * i : at + 8 * i + 8, :] for i in range(width)]
        ends = got[-1]
        out = []
        for g in range(quads):
            one, two, three = got[3 * g : 3 * g + 3]
            four = jnp.where(
                lane < quarter, pltpu.roll(one, quarter, 1),
                jnp.where(lane < 2 * quarter, pltpu.roll(two, 2 * quarter, 1),
                          pltpu.roll(three, 3 * quarter, 1)),
            )
            for x in (one, two, three, four):
                spots = [p for p, _ in end_spots(j, len(out), x)]
                x = jnp.take_along_axis(x, inner[which], axis=1)
                parts = [jnp.broadcast_to(ends[:, p : p + 1], (8, columns)) for p in spots]
                end = parts[0]
                if len(parts) > 1:
                    end = jnp.where(sublane < 4, end, pltpu.roll(parts[1], 4, 0))
                out.append(jnp.where(rim_end[which], end, x))
        for x in got[3 * quads :]:
            out.append(jnp.take_along_axis(x, spread[which], axis=1))
        if j >= heat:
            second = pltpu.roll(out[-1], 8 - tail, 0)
            out = out[:full] + out[-1:] + out[full : 2 * full] + [second]
        return out

    sets = [[0], [1, 2, 3, heat], [4, last, last], [5]]
    corner_spot = {j: (w, group.index(j)) for w, group in enumerate(sets) for j in group}

    def sides_of(j):
        p = first_pack[j]
        if j < last:
            return [sides(p)]
        xu, xv = sides(p), sides(p + 1)
        return [side_cos * xu - side_sin * xv, side_sin * xu + side_cos * xv]

    def with_corners(j):
        which, p = corner_spot[j]
        if j < last:
            return [seam_x[first_pack[j]] + sum_corners(which, p)]
        xu, xv = seam_x[first_pack[j]], seam_x[first_pack[j] + 1]
        for d in range(4):
            cu, cv = corner_values(which, d, p), corner_values(which, d, p + 1)
            c, s = cosine(corner_code[d]), sine(corner_code[d])
            xu, xv = xu + (c * cu - s * cv), xv + (s * cu + c * cv)
        return [xu, xv]

    def sum_corners(which, p):
        parts = [corner_values(which, d, p) for d in range(4)]
        return parts[0] + parts[1] + parts[2] + parts[3]

    def rims_of(j):
        both = [row_rim(up_in, 0, j), row_rim(down_in, 1, j)]
        if j == last:
            for which in range(2):
                x = both[which]
                c, s = cosine(codes[which]), sine(codes[which])
                ru = [c * x[i] - s * x[groups + i] for i in range(groups)]
                rv = [s * x[i] + c * x[groups + i] for i in range(groups)]
                both[which] = ru + rv
        return both

    def stored(ref, begin, i, valid, r, x):
        n = min(8, valid - 8 * i)
        for a in range(rows):
            if rep[a] == r:
                ref[pl.ds((begin + 8 * i) * rows + a, n, stride=rows), :] = (x * inverse[a])[:n]

    inverse = [None] * rows

    def finish(j, seams, which_rows, both=None):
        start, total_count, packs = pieces[j]
        each = (total_count // packs) // 8
        for i in range(total_count // 8):
            for r in which_rows:
                x = z_ref[r, start + 8 * i : start + 8 * i + 8, :]
                x = x + to_edges(seams[i // each], i % each, r)
                if r in borders:
                    x = x + both[0 if r == 0 else 1][i]
                if j == 0:
                    for a in range(rows):
                        if rep[a] == r:
                            inverse[a] = 1.0 / x
                elif j < heat:
                    begin, _, valid = chunks[j - 1]
                    stored(tracer_o, begin, i, valid, r, x)
                else:
                    first_half, k = i < groups, i % groups
                    if j == heat:
                        ref = temp_o if first_half else thick_o
                    else:
                        ref = wind_o.at[0 if first_half else 1]
                    stored(ref, 0, k, levels, r, x)

    groups = pad // 8
    def finish_insides(order):
        for j in order:
            drain(2 * side_rows[j], side_sem.at[j])
        for j in order:
            seams = sides_of(j)
            for i, x in enumerate(seams):
                seam_x[first_pack[j] + i] = x
            finish(j, seams, insides)

    def finish_borders(order, corners):
        for j in order:
            drain(2 * packed[j][2], piece_sem.at[j])
        for which in corners:
            drain(16 if which else 4, corner_sem.at[which])
        for j in order:
            finish(j, with_corners(j), borders, rims_of(j))

    finish_insides([0, 1, 2, 3, heat, 4])
    peak[1] = gathered(0, 0, len(plane))
    for o in range(1, nf):
        send(peak.at[1, pl.ds(0, 2)], peak_in.at[len(plane) + o - 1, pl.ds(0, 2)],
             peak_sem.at[1], (lax.rem(face + o, nf), tile, lev))
    finish_borders([0, 1, 2, 3, heat], [0, 1])
    finish_insides([last, 5])
    finish_borders([4, last], [2])
    finish_borders([5], [3])

    bound_o[...] = gathered(1, len(plane), nf - 1)
    drain(sum(sent), sent_sem.at[0])


def write_out(wind, temp, thick, tracer, bound, wind_o, temp_o, thick_o, tracer_o, bound_o, pair, sem):
    pairs = ((tracer, tracer_o), (wind, wind_o), (temp, temp_o), (thick, thick_o))
    copies = [pltpu.make_async_copy(a, b, sem.at[i]) for i, (a, b) in enumerate(pairs)]
    for copy in copies:
        copy.start()
    pair[0] = jnp.max(bound[0:1, :])
    pair[1] = jnp.max(bound[1:2, :])
    copies.append(pltpu.make_async_copy(pair, bound_o, sem.at[4]))
    copies[-1].start()
    for copy in copies:
        copy.wait()


def on_device(
    sizes, wind, temp, thick, tracers, ground, maps, det, rot, flip, tally
):
    nf, nt, nl = sizes
    levels, rows, columns = temp.shape
    count = tracers.shape[0]
    chunks = layout(levels, count)
    pad = -(-levels // 8) * 8
    if rows != 8 or columns != 128 or levels % 8 not in (1, 2, 3, 4) or len(chunks) != 5:
        raise ValueError("block shape")
    table, dct, w_col = lane_tables(columns)
    distinct = rows - rows // 4 + 1
    total_rows = 4 * pad + 8 + sum(c[1] for c in chunks)
    pieces = len(chunks) + 3
    packs = len(chunks) + 4
    landing = sum(8 * p[1] for p in packing(levels, chunks))
    whole = max(c[1] for c in chunks)
    n = levels * rows
    dma = pltpu.SemaphoreType.DMA
    peers = nt * nl - 1 + nf - 1
    hbm = pl.BlockSpec(memory_space=pl.ANY)
    smem = pl.BlockSpec(memory_space=pltpu.SMEM)
    vmem = pl.BlockSpec(memory_space=pltpu.VMEM)
    last = chunks[-1]
    shapes = ((2, n, columns), (n, columns), (n, columns), (count * n, columns), (8, columns))
    outs = pl.pallas_call(
        functools.partial(kernel, sizes, (levels, rows, columns, chunks, pad)),
        out_shape=tuple(pltpu.VMEM(shape, f32) for shape in shapes),
        in_specs=[hbm] * 13,
        out_specs=(vmem,) * 5,
        scratch_shapes=[
            pltpu.VMEM((2, pad * rows, columns), f32),
            pltpu.VMEM((pad * rows, columns), f32),
            pltpu.VMEM((pad * rows, columns), f32),
            pltpu.VMEM(((last[0] + last[1]) * rows, columns), f32),
            pltpu.VMEM((pad * rows, columns), f32),
            pltpu.VMEM((rows, columns), f32),
            pltpu.VMEM((4 * rows, columns), f32),
            pltpu.VMEM((rows, columns), f32),
            pltpu.VMEM(table.shape, bf16),
            pltpu.VMEM(dct.shape, bf16),
            pltpu.VMEM((1, columns), f32),
            pltpu.VMEM((rows, whole, columns), f32),
            pltpu.VMEM((rows, whole, columns), f32),
            pltpu.VMEM((distinct, total_rows, columns), f32),
            pltpu.VMEM((landing, columns), f32),
            pltpu.VMEM((landing, columns), f32),
            pltpu.VMEM((packs, 8, columns), f32),
            pltpu.VMEM((packs, 8, columns), f32),
            pltpu.VMEM((4, 4, 8, columns), f32),
            pltpu.VMEM((rows, columns), f32),
            pltpu.VMEM((3, 8, columns), f32),
            pltpu.VMEM((landing, columns), f32),
            pltpu.VMEM((landing, columns), f32),
            pltpu.VMEM((packs, 8, columns), f32),
            pltpu.VMEM((packs, 8, columns), f32),
            pltpu.VMEM((4, 4, 8, columns), f32),
            pltpu.VMEM((nl - 1, rows, columns), f32),
            pltpu.VMEM((peers, 8, columns), f32),
            pltpu.SMEM((nf, 2, nt), jnp.int32),
            pltpu.SMEM((nf, 2, nt), jnp.int32),
            pltpu.SMEM((nf, nt), jnp.int32),
            dma((7 + len(chunks),)),
            dma((1,)),
            dma((pieces,)),
            dma((pieces,)),
            dma((4,)),
            dma((1,)),
            dma((3,)),
            pltpu.SemaphoreType.REGULAR((2,)),
        ],
        compiler_params=pltpu.CompilerParams(collective_id=0, has_side_effects=True),
    )(
        wind.reshape(2, n, columns), temp.reshape(n, columns), thick.reshape(n, columns),
        tracers.reshape(count * n, columns), ground, maps.reshape(4 * rows, columns), det,
        table, dct, w_col, rot.transpose(0, 2, 1), flip.transpose(0, 2, 1), tally,
    )
    outs = pl.pallas_call(
        write_out,
        out_shape=tuple(jax.ShapeDtypeStruct(x, f32) for x in shapes[:4] + ((2,),)),
        in_specs=[vmem] * 5,
        out_specs=(hbm,) * 5,
        scratch_shapes=[pltpu.SMEM((2,), f32), dma((5,))],
    )(*[pltpu.with_memory_space_constraint(x, pltpu.VMEM) for x in outs])
    return (
        outs[0].reshape(wind.shape), outs[1].reshape(temp.shape), outs[2].reshape(thick.shape),
        outs[3].reshape(tracers.shape), outs[4],
    )


def solution(mesh):
    sizes = tuple(mesh.shape[name] for name in ("face", "tile", "lev"))
    level = P("lev", "face", "tile")
    stacked = P(None, "lev", "face", "tile")
    return jax.shard_map(
        functools.partial(on_device, sizes),
        mesh=mesh,
        in_specs=(stacked, level, level, stacked, P("face", "tile"), P(None, "face", "tile"),
                  P("face", "tile"), P(), P(), P()),
        out_specs=(stacked, level, level, stacked, P()),
        check_vma=False,
    )
```
